8 devices in a mesh: dp: 1 (over z), ep: 8 (over y, x, core).
Axes of the slice: x: 2, y: 2, z: 1, core: 2. Of those that a mesh axis runs over, the one named last changes fastest.
Arguments:
- resid_in: bfloat16 [2, 32, 384, 2048], P(None, ('dp', 'ep'))
- expert_idx: int32 [2, 32, 384, 6], P(None, ('dp', 'ep'))
- expert_slot: int32 [2, 32, 384, 6], P(None, ('dp', 'ep'))
- w_query: bfloat16 [2048, 16, 128], replicated
- w_key: bfloat16 [2048, 16, 128], replicated
- w_value: bfloat16 [2048, 16, 128], replicated
- w_out: bfloat16 [16, 128, 2048], replicated
- w_gate: bfloat16 [2048, 10944], replicated
- w_up: bfloat16 [2048, 10944], replicated
- w_down: bfloat16 [10944, 2048], replicated
- w_router: bfloat16 [2048, 64], replicated
- norm_attn: bfloat16 [2048], replicated
- norm_ffn: bfloat16 [2048], replicated
- norm_moe: bfloat16 [2048], replicated
- expert_gate: bfloat16 [64, 2048, 1408], P('ep')
- expert_up: bfloat16 [64, 2048, 1408], P('ep')
- expert_down: bfloat16 [64, 1408, 2048], P('ep')
Outputs:
- output: bfloat16 [2, 32, 384, 2048], P(None, ('dp', 'ep'))
All inputs are finite; a program needn't handle non-finite values.
Results may differ from the reference program's by a relative error of at most 0.00994233.
Values are sent between devices in bfloat16 or wider.
A program may use at most 1.25 GiB of HBM per device.

```python
import jax
import jax.numpy as jnp
from jax import lax

D = 2048
HEADS = 16
KV_HEADS = 16
HEAD = 128
EXPERTS = 64
TOP = 6
FE = 1408
FF = 10944
SEQ = 384
SEQS = 4
GROUP = 8

TOK_MB = SEQS * SEQ
CAP = 2 * TOK_MB * TOP // EXPERTS
EPS = 1e-6
ROPE_BASE = 10000.0


def draw_device(rng_key):
    count_key, label_key, order_key = jax.random.split(rng_key, 3)
    pair_left = jax.random.randint(count_key, (EXPERTS // 2,), 0, CAP + 1)
    pair_left = pair_left.at[0].set(CAP)
    counts = jnp.stack([pair_left, CAP - pair_left], axis=1).reshape(EXPERTS)
    count_ends = jnp.cumsum(counts)
    count_starts = count_ends - counts
    copy_pos = jnp.arange(TOK_MB * TOP)
    sorted_ids = jnp.sum(copy_pos[:, None] >= count_ends[None, :], axis=1)
    slot_ranks = copy_pos - count_starts[sorted_ids]
    labels = jax.random.permutation(label_key, EXPERTS)[sorted_ids]
    token_order = jax.random.permutation(order_key, TOK_MB)
    ids_out = labels.reshape(TOP, TOK_MB).T[token_order]
    slots_out = slot_ranks.reshape(TOP, TOK_MB).T[token_order]
    return ids_out.astype(jnp.int32), slots_out.astype(jnp.int32)


def draw_routing(rng_key):
    device_keys = jax.random.split(rng_key, 2 * GROUP)
    ids_all, slots_all = jax.vmap(draw_device)(device_keys)
    return (ids_all.reshape(2, GROUP * SEQS, SEQ, TOP), slots_all.reshape(2, GROUP * SEQS, SEQ, TOP))


def setup_inputs(seed: int = 0, part: int = 0) -> dict:
    root_key = jax.random.key(seed)
    weight_keys = jax.random.split(root_key, 14)
    part_key = jax.random.fold_in(jax.random.key(seed + 1), part)
    act_key, route_key = jax.random.split(part_key)

    def normal_weight(rng_key, shape, fan_in, gain):
        raw_draw = jax.random.normal(rng_key, shape, jnp.float32)
        return (raw_draw * (gain * fan_in ** -0.5)).astype(jnp.bfloat16)

    def norm_scale(rng_key):
        return (1.0 + 0.3 * jax.random.normal(rng_key, (D,), jnp.float32)).astype(jnp.bfloat16)

    resid_in = jax.random.normal(act_key, (2, GROUP * SEQS, SEQ, D), jnp.float32).astype(jnp.bfloat16)
    expert_idx, expert_slot = draw_routing(route_key)
    return {
        'resid_in': resid_in,
        'expert_idx': expert_idx,
        'expert_slot': expert_slot,
        'w_query': normal_weight(weight_keys[0], (D, HEADS, HEAD), D, 2.0),
        'w_key': normal_weight(weight_keys[1], (D, KV_HEADS, HEAD), D, 1.0),
        'w_value': normal_weight(weight_keys[2], (D, KV_HEADS, HEAD), D, 1.0),
        'w_out': normal_weight(weight_keys[3], (HEADS, HEAD, D), HEADS * HEAD, 2.0),
        'w_gate': normal_weight(weight_keys[4], (D, FF), D, 1.0),
        'w_up': normal_weight(weight_keys[5], (D, FF), D, 1.0),
        'w_down': normal_weight(weight_keys[6], (FF, D), FF, 1.0),
        'w_router': normal_weight(weight_keys[7], (D, EXPERTS), D, 2.0),
        'norm_attn': norm_scale(weight_keys[8]),
        'norm_ffn': norm_scale(weight_keys[9]),
        'norm_moe': norm_scale(weight_keys[10]),
        'expert_gate': normal_weight(weight_keys[11], (EXPERTS, D, FE), D, 1.0),
        'expert_up': normal_weight(weight_keys[12], (EXPERTS, D, FE), D, 1.0),
        'expert_down': normal_weight(weight_keys[13], (EXPERTS, FE, D), FE, 2.0),
    }


def rms_norm(values, scale):
    widened = values.astype(jnp.float32)
    mean_sq = jnp.mean(widened * widened, axis=-1, keepdims=True)
    return (widened * lax.rsqrt(mean_sq + EPS) * scale.astype(jnp.float32)).astype(jnp.bfloat16)


def rotary(values):
    half_dim = HEAD // 2
    freqs = ROPE_BASE ** (-jnp.arange(half_dim, dtype=jnp.float32) * 2.0 / HEAD)
    angles = jnp.arange(SEQ, dtype=jnp.float32)[:, None] * freqs[None, :]
    cosine = jnp.cos(angles)[:, None, :]
    sine = jnp.sin(angles)[:, None, :]
    first = values[..., :half_dim]
    second = values[..., half_dim:]
    return jnp.concatenate([first * cosine - second * sine, second * cosine + first * sine], axis=-1)


def swiglu(normed, w_gate, w_up, w_down):
    gate_act = jnp.dot(normed, w_gate, preferred_element_type=jnp.float32)
    up_act = jnp.dot(normed, w_up, preferred_element_type=jnp.float32)
    hidden = (jax.nn.silu(gate_act) * up_act).astype(jnp.bfloat16)
    return jnp.dot(hidden, w_down, preferred_element_type=jnp.float32)


def reference(resid_in, expert_idx, expert_slot, w_query, w_key, w_value, w_out, w_gate, w_up, w_down, w_router, norm_attn, norm_ffn, norm_moe, expert_gate, expert_up, expert_down):
    group_heads = HEADS // KV_HEADS
    causal = jnp.arange(SEQ)[:, None] >= jnp.arange(SEQ)[None, :]
    query_flat = w_query.reshape(D, HEADS * HEAD)
    key_flat = w_key.reshape(D, KV_HEADS * HEAD)
    value_flat = w_value.reshape(D, KV_HEADS * HEAD)
    out_flat = w_out.reshape(HEADS * HEAD, D)

    def dense_sequence(resid):
        normed = rms_norm(resid, norm_attn)
        queries = rotary(jnp.dot(normed, query_flat, preferred_element_type=jnp.float32).reshape(SEQ, HEADS, HEAD)).astype(jnp.bfloat16)
        keys_rot = rotary(jnp.dot(normed, key_flat, preferred_element_type=jnp.float32).reshape(SEQ, KV_HEADS, HEAD)).astype(jnp.bfloat16)
        values_in = jnp.dot(normed, value_flat, preferred_element_type=jnp.float32).astype(jnp.bfloat16).reshape(SEQ, KV_HEADS, HEAD)
        keys_rep = jnp.repeat(keys_rot, group_heads, axis=1)
        values_rep = jnp.repeat(values_in, group_heads, axis=1)
        scores = jnp.einsum('qhe,khe->hqk', queries.astype(jnp.float32), keys_rep.astype(jnp.float32)) * (HEAD ** -0.5)
        probs = jax.nn.softmax(jnp.where(causal[None], scores, -1e30), axis=-1).astype(jnp.bfloat16)
        attended = jnp.einsum('hqk,khe->qhe', probs.astype(jnp.float32), values_rep.astype(jnp.float32)).astype(jnp.bfloat16)
        attn_out = jnp.dot(attended.reshape(SEQ, HEADS * HEAD), out_flat, preferred_element_type=jnp.float32)
        after_attn = (resid.astype(jnp.float32) + attn_out).astype(jnp.bfloat16)
        ffn_out = swiglu(rms_norm(after_attn, norm_ffn), w_gate, w_up, w_down)
        return after_attn.astype(jnp.float32) + ffn_out

    token_count = 2 * GROUP * TOK_MB
    dense_out = lax.map(dense_sequence, resid_in.reshape(2 * GROUP * SEQS, SEQ, D)).reshape(token_count, D)

    normed_moe = rms_norm(resid_in.reshape(token_count, D), norm_moe)
    logits = jnp.dot(normed_moe, w_router, preferred_element_type=jnp.float32)
    route_ids = expert_idx.reshape(token_count, TOP)
    route_slots = expert_slot.reshape(token_count, TOP)
    gates = jax.nn.softmax(jnp.take_along_axis(logits, route_ids, axis=1), axis=-1)
    token_pos = jnp.arange(token_count, dtype=jnp.int32)
    micro_of = token_pos // (GROUP * TOK_MB)
    device_of = (token_pos // TOK_MB) % GROUP
    buf_pos = ((route_ids * 2 + micro_of[:, None]) * GROUP + device_of[:, None]) * CAP + route_slots
    copy_count = token_count * TOP
    copy_of_row = jnp.full((EXPERTS * 2 * GROUP * CAP,), copy_count, jnp.int32)
    copy_of_row = copy_of_row.at[buf_pos.reshape(-1)].set(jnp.arange(copy_count, dtype=jnp.int32))
    copy_of_row = copy_of_row.reshape(EXPERTS, 2 * GROUP * CAP)
    gate_flat = gates.reshape(copy_count)

    def expert_step(accum_out, expert_args):
        w_a, w_b, w_c, row_copies = expert_args
        row_tokens = row_copies // TOP
        rows_in = jnp.take(normed_moe, row_tokens, axis=0, mode='fill', fill_value=0)
        expert_out = swiglu(rows_in, w_a, w_b, w_c).astype(jnp.bfloat16)
        row_gates = jnp.take(gate_flat, row_copies, mode='fill', fill_value=0)
        accum_out = accum_out.at[row_tokens].add(row_gates[:, None] * expert_out.astype(jnp.float32), mode='drop')
        return accum_out, None

    moe_out = lax.scan(expert_step, jnp.zeros((token_count, D), jnp.float32), (expert_gate, expert_up, expert_down, copy_of_row))[0]
    return (dense_out + moe_out).astype(jnp.bfloat16).reshape(2, GROUP * SEQS, SEQ, D)
```

```python
import jax
import jax.numpy as jnp
from jax import lax
from jax.sharding import PartitionSpec as P

EPS = 1e-6
ROPE_BASE = 10000.0
CAP_FACTOR = 2
NEG = -1e30


def rms_norm(values, scale):
    widened = values.astype(jnp.float32)
    mean_sq = jnp.mean(widened * widened, axis=-1, keepdims=True)
    return (widened * lax.rsqrt(mean_sq + EPS) * scale.astype(jnp.float32)).astype(jnp.bfloat16)


def rotary(values):
    seq_len = values.shape[-3]
    head_dim = values.shape[-1]
    half_dim = head_dim // 2
    freqs = ROPE_BASE ** (-jnp.arange(half_dim, dtype=jnp.float32) * 2.0 / head_dim)
    angles = jnp.arange(seq_len, dtype=jnp.float32)[:, None] * freqs[None, :]
    cosine = jnp.cos(angles)[:, None, :]
    sine = jnp.sin(angles)[:, None, :]
    first = values[..., :half_dim]
    second = values[..., half_dim:]
    return jnp.concatenate([first * cosine - second * sine, second * cosine + first * sine], axis=-1)


def dense_branch(resid, norm_attn, w_query, w_key, w_value, w_out, norm_ffn, w_gate, w_up, w_down):
    batch, seq_len = resid.shape[0], resid.shape[1]
    heads, head_dim = w_query.shape[1], w_query.shape[2]
    kv_heads = w_key.shape[1]
    normed = rms_norm(resid, norm_attn)
    queries = rotary(jnp.einsum('bsd,dhe->bshe', normed, w_query, preferred_element_type=jnp.float32)).astype(jnp.bfloat16)
    keys_rot = rotary(jnp.einsum('bsd,dhe->bshe', normed, w_key, preferred_element_type=jnp.float32)).astype(jnp.bfloat16)
    values_in = jnp.einsum('bsd,dhe->bshe', normed, w_value, preferred_element_type=jnp.float32).astype(jnp.bfloat16)
    grouped = queries.reshape(batch, seq_len, kv_heads, heads // kv_heads, head_dim)
    scores = jnp.einsum('bqgre,bkge->bgrqk', grouped, keys_rot, preferred_element_type=jnp.float32) * (head_dim ** -0.5)
    causal = jnp.arange(seq_len)[:, None] >= jnp.arange(seq_len)[None, :]
    probs = jax.nn.softmax(jnp.where(causal, scores, NEG), axis=-1).astype(jnp.bfloat16)
    attended = jnp.einsum('bgrqk,bkge->bqgre', probs, values_in, preferred_element_type=jnp.float32).astype(jnp.bfloat16)
    attn_out = jnp.einsum('bshe,hed->bsd', attended.reshape(batch, seq_len, heads, head_dim), w_out, preferred_element_type=jnp.float32)
    after_attn = (resid.astype(jnp.float32) + attn_out).astype(jnp.bfloat16)
    normed_ffn = rms_norm(after_attn, norm_ffn)
    gate_act = jnp.einsum('bsd,df->bsf', normed_ffn, w_gate, preferred_element_type=jnp.float32)
    up_act = jnp.einsum('bsd,df->bsf', normed_ffn, w_up, preferred_element_type=jnp.float32)
    hidden = (jax.nn.silu(gate_act) * up_act).astype(jnp.bfloat16)
    down_act = jnp.einsum('bsf,fd->bsd', hidden, w_down, preferred_element_type=jnp.float32)
    return after_attn.astype(jnp.float32) + down_act


def expert_ffn(rows_in, expert_gate, expert_up, expert_down):
    gate_act = jnp.einsum('lrd,ldf->lrf', rows_in, expert_gate, preferred_element_type=jnp.float32)
    up_act = jnp.einsum('lrd,ldf->lrf', rows_in, expert_up, preferred_element_type=jnp.float32)
    hidden = (jax.nn.silu(gate_act) * up_act).astype(jnp.bfloat16)
    return jnp.einsum('lrf,lfd->lrd', hidden, expert_down, preferred_element_type=jnp.float32).astype(jnp.bfloat16)


def solution(mesh):
    group_size = mesh.shape['ep']
    tok_spec = P(None, ('dp', 'ep'), None, None)
    rep_one = P(None)
    rep_two = P(None, None)
    rep_three = P(None, None, None)
    expert_spec = P('ep', None, None)
    chips = group_size // 2
    same_core = [[2 * c for c in range(chips)], [2 * c + 1 for c in range(chips)]]
    partner = [(i, i ^ 1) for i in range(group_size)]

    def local_program(resid_in, expert_idx, expert_slot, w_query, w_key, w_value, w_out, w_gate, w_up, w_down, w_router, norm_attn, norm_ffn, norm_moe, expert_gate, expert_up, expert_down):
        micro_count, seqs, seq_len, width = resid_in.shape
        tokens = seqs * seq_len
        choices = expert_idx.shape[-1]
        local_experts = expert_gate.shape[0]
        experts = local_experts * group_size
        capacity = CAP_FACTOR * tokens * choices // experts
        me = lax.axis_index('ep')
        gate_all = jnp.stack([expert_gate, lax.ppermute(expert_gate, 'ep', partner)])
        up_all = jnp.stack([expert_up, lax.ppermute(expert_up, 'ep', partner)])
        down_all = jnp.stack([expert_down, lax.ppermute(expert_down, 'ep', partner)])
        own_first = me * local_experts
        other_first = (me ^ 1) * local_experts

        def mine(table, axis):
            return jnp.concatenate([lax.dynamic_slice_in_dim(table, own_first, local_experts, axis), lax.dynamic_slice_in_dim(table, other_first, local_experts, axis)], axis)

        outputs = []
        for micro in range(micro_count):
            resid = resid_in[micro]
            ids = expert_idx[micro].reshape(tokens, choices)
            normed = rms_norm(resid.reshape(tokens, width), norm_moe)
            logits = jnp.dot(normed, w_router, preferred_element_type=jnp.float32)
            picked = jnp.any(ids[:, :, None] == jnp.arange(experts)[None, None, :], axis=1)
            gates = jax.nn.softmax(jnp.where(picked, logits, NEG), axis=-1) * picked
            lower = (jnp.arange(tokens)[:, None] >= jnp.arange(tokens)[None, :]).astype(jnp.bfloat16)
            upto = jnp.dot(lower, picked.astype(jnp.bfloat16), preferred_element_type=jnp.float32)
            tok_of = jnp.sum((upto.T[:, None, :] <= jnp.arange(capacity, dtype=jnp.float32)[None, :, None]).astype(jnp.int32), axis=-1)
            all_tok = lax.all_gather(normed, 'ep', axis_index_groups=same_core)
            all_tab = mine(lax.all_gather(tok_of, 'ep', axis_index_groups=same_core), 1)
            all_gates = mine(lax.all_gather(gates, 'ep', axis_index_groups=same_core), 2)
            all_upto = mine(lax.all_gather(jnp.where(picked, upto, 0.0), 'ep', axis_index_groups=same_core), 2)
            row_tok = jnp.where(all_tab < tokens, all_tab + jnp.arange(chips)[:, None, None] * tokens, 0)
            rows = jnp.take(all_tok.reshape(chips * tokens, width), row_tok.transpose(1, 0, 2).reshape(-1), axis=0)
            rows = rows.reshape(2, local_experts, chips * capacity, width)
            y = jnp.stack([expert_ffn(rows[0], gate_all[0], up_all[0], down_all[0]), expert_ffn(rows[1], gate_all[1], up_all[1], down_all[1])])
            y = y.reshape(2 * local_experts * chips * capacity, width)
            here = all_upto > 0
            order = jnp.cumsum(here.astype(jnp.int32), axis=-1)
            part = jnp.zeros((chips * tokens, width), jnp.float32)
            row_id = (jnp.arange(2 * local_experts)[None, None, :] * chips + jnp.arange(chips)[:, None, None]) * capacity + all_upto.astype(jnp.int32) - 1
            for j in range(choices):
                hit = here & (order == j + 1)
                rj = jnp.sum(jnp.where(hit, row_id, 0), axis=-1).reshape(-1)
                gj = jnp.sum(jnp.where(hit, all_gates, 0.0), axis=-1).reshape(-1)
                part = part + gj[:, None] * jnp.take(y, rj, axis=0).astype(jnp.float32)
            moe_out = lax.psum_scatter(part.reshape(chips, tokens, width), 'ep', scatter_dimension=0, axis_index_groups=same_core)
            dense_out = dense_branch(resid, norm_attn, w_query, w_key, w_value, w_out, norm_ffn, w_gate, w_up, w_down)
            outputs.append((dense_out + moe_out.reshape(seqs, seq_len, width)).astype(jnp.bfloat16))
        return jnp.stack(outputs)

    return jax.shard_map(local_program, mesh=mesh, in_specs=(tok_spec, tok_spec, tok_spec, rep_three, rep_three, rep_three, rep_three, rep_two, rep_two, rep_two, rep_two, rep_one, rep_one, rep_one, expert_spec, expert_spec, expert_spec), out_specs=tok_spec, check_vma=False)
```

```python
import functools

import jax
import jax.numpy as jnp
from jax import lax
from jax.experimental import pallas as pl
from jax.experimental.pallas import tpu as pltpu
from jax.sharding import PartitionSpec as P

EPS = 1e-6
ROPE_BASE = 10000.0
CAP_FACTOR = 2
NEG = -1e30
LANES = 128
PITCH = 9
F32 = jnp.float32
BF16 = jnp.bfloat16


def rms_norm(values, scale):
    widened = values.astype(F32)
    mean_sq = jnp.mean(widened * widened, axis=-1, keepdims=True)
    return (widened * lax.rsqrt(mean_sq + EPS) * scale.astype(F32)).astype(BF16)


def ffn_branch(after_attn, norm_ffn, w_gate, w_up, w_down):
    normed_ffn = rms_norm(after_attn, norm_ffn)
    gate_act = jnp.dot(normed_ffn, w_gate, preferred_element_type=F32)
    up_act = jnp.dot(normed_ffn, w_up, preferred_element_type=F32)
    hidden = (gate_act * jax.nn.sigmoid(gate_act) * up_act).astype(BF16)
    return after_attn.astype(F32) + jnp.dot(hidden, w_down, preferred_element_type=F32)


def expert_kernel(cfg, cnt, tok, u, wg0, wu0, wd0, wg1, wu1, wd1, y, wg, wu, wd, x3, xs, x2, h, yb, wsem, xsem, ysem):
    E, S, CAP, KB, FE, MAXR, BIG = cfg
    half = E // 2
    D = KB * LANES

    def weights(e, slot, start):
        if not start:
            pltpu.make_async_copy(wg0.at[0], wg.at[slot], wsem.at[slot]).wait()
            pltpu.make_async_copy(wu0.at[0], wu.at[slot], wsem.at[slot]).wait()
            pltpu.make_async_copy(wd0.at[0], wd.at[slot], wsem.at[slot]).wait()
            return

        @pl.when(e < half)
        def _():
            pltpu.make_async_copy(wg0.at[e], wg.at[slot], wsem.at[slot]).start()
            pltpu.make_async_copy(wu0.at[e], wu.at[slot], wsem.at[slot]).start()
            pltpu.make_async_copy(wd0.at[e], wd.at[slot], wsem.at[slot]).start()

        @pl.when(e >= half)
        def _():
            pltpu.make_async_copy(wg1.at[e - half], wg.at[slot], wsem.at[slot]).start()
            pltpu.make_async_copy(wu1.at[e - half], wu.at[slot], wsem.at[slot]).start()
            pltpu.make_async_copy(wd1.at[e - half], wd.at[slot], wsem.at[slot]).start()

    def rows_of(e):
        total = 0
        for s in range(S):
            total = total + (cnt[s * E + e] + 7) // 8
        return total

    def gather(e, slot):
        pos = slot * MAXR
        for s in range(S):
            groups = (cnt[s * E + e] + 7) // 8
            base = (s * E + e) * CAP

            def issue(i, carry, pos=pos, base=base):
                for k in range(8):
                    t = tok[base + i * 8 + k]
                    pltpu.make_async_copy(u.at[t], x3.at[pos + i * 8 + k], xsem.at[slot]).start()
                return carry

            lax.fori_loop(0, groups, issue, 0)
            pos = pos + groups * 8

    def gather_wait(e, slot):
        def one(i, carry):
            pltpu.make_async_copy(u.at[pl.ds(0, 8)], x3.at[pl.ds(0, 8)], xsem.at[slot]).wait()
            return carry

        lax.fori_loop(0, rows_of(e), one, 0)

    def y_wait(rows, ys):
        pltpu.make_async_copy(yb.at[ys, pl.ds(0, rows // 8 * KB * PITCH)], y.at[pl.ds(0, rows // 8 * KB * PITCH)], ysem.at[ys]).wait()

    def block(e, slot, r0, M, ys):
        src = slot * MAXR + r0

        def relayout(g, carry):
            for i in range(32):
                xs[i * (KB + 1):i * (KB + 1) + KB, :] = x3[src + g * 32 + i].astype(F32)
            for half in range(2):
                for k in range(KB):
                    x2[g * 2 + half, k] = xs[pl.ds(half * 16 * (KB + 1) + k, 16, stride=KB + 1), :].astype(BF16)
            return carry

        lax.fori_loop(0, M // 32, relayout, 0)
        x = jnp.concatenate([x2[0:M // 16, k].reshape(M, LANES) for k in range(KB)], axis=1)
        full = FE // 256
        for j in range(full):
            cols = slice(j * 256, j * 256 + 256)
            ga = jnp.dot(x, wg[slot, :, cols], preferred_element_type=F32)
            ua = jnp.dot(x, wu[slot, :, cols], preferred_element_type=F32)
            h[0:M, cols] = (ga * jax.nn.sigmoid(ga) * ua).astype(BF16)
        if FE % 256:
            cols = slice(full * 256, FE)
            width = FE - full * 256
            both = jnp.dot(x, jnp.concatenate([wg[slot, :, cols], wu[slot, :, cols]], axis=1), preferred_element_type=F32)
            ga, ua = both[:, :width], both[:, width:]
            h[0:M, cols] = (ga * jax.nn.sigmoid(ga) * ua).astype(BF16)
        hid = h[0:M, :]
        for j in range(D // 256):
            out = jnp.dot(hid, wd[slot, :, j * 256:j * 256 + 256], preferred_element_type=F32)
            out = out.astype(BF16).astype(F32)
            for rb in range(M // 8):
                for k in range(2):
                    at = (rb * KB + 2 * j + k) * PITCH
                    yb[ys, at:at + 8, :] = out[rb * 8:rb * 8 + 8, k * LANES:(k + 1) * LANES]
        dst = pl.multiple_of((e * MAXR + r0) // 8 * (KB * PITCH), 8)
        pltpu.make_async_copy(yb.at[ys, pl.ds(0, M // 8 * KB * PITCH)], y.at[pl.ds(dst, M // 8 * KB * PITCH)], ysem.at[ys]).start()

    small = 2 * BIG // 3
    unit = BIG // 3
    weights(0, 0, True)
    gather(0, 0)

    def per_expert(e, carry):
        slot = lax.rem(e, 2)
        weights(e, slot, False)
        gather_wait(e, slot)

        @pl.when(e + 1 < E)
        def _():
            weights(e + 1, 1 - slot, True)
            gather(e + 1, 1 - slot)

        units = (rows_of(e) * 8 + unit - 1) // unit
        odd = jnp.logical_and(lax.rem(units, 2) == 1, units >= 3).astype(jnp.int32)
        pairs = (units - 3 * odd + 1) // 2

        @pl.when(odd == 1)
        def _():
            block(e, slot, 0, BIG, 0)
            y_wait(BIG, 0)

        def pair(i, c):
            block(e, slot, pl.multiple_of(odd * BIG + i * small, unit), small, 1)
            y_wait(small, 1)
            return c

        lax.fori_loop(0, pairs, pair, 0)
        return carry

    lax.fori_loop(0, E, per_expert, 0)


def combine_kernel(cfg, cnt, pos, addr, gate, y, part, acc, ybuf, ysem, osem):
    E, S, CAP, KB, MAXR, T, DEPTH = cfg
    PIECE = 32
    seg_rows = CAP // 8 * KB * PITCH
    piece_rows = PIECE // 8 * KB * PITCH

    def fetch(q, start):
        slot = lax.rem(q, DEPTH)
        s = q // E
        e = q - s * E
        pieces = (cnt[q] + PIECE - 1) // PIECE
        base = pl.multiple_of((e * MAXR + pos[q]) // 8 * (KB * PITCH), 8)

        def one(i, c):
            src = y.at[pl.ds(pl.multiple_of(base + i * piece_rows, 8), piece_rows)]
            dst = ybuf.at[pl.ds(pl.multiple_of(slot * seg_rows + i * piece_rows, 8), piece_rows)]
            copy = pltpu.make_async_copy(src, dst, ysem.at[slot])
            copy.start() if start else copy.wait()
            return c

        lax.fori_loop(0, pieces, one, 0)

    for q in range(DEPTH - 1):
        fetch(q, True)
    zero = jnp.zeros((8 * KB, LANES), F32)
    for s in range(S):
        a = s % 2
        if s >= 2:
            pltpu.make_async_copy(acc.at[a, pl.ds(0, T * KB)], part.at[s - 2], osem.at[a]).wait()

        def clear(i, c):
            acc[a, pl.ds(pl.multiple_of(i * 8 * KB, 8), 8 * KB), :] = zero
            return c

        lax.fori_loop(0, T // 8, clear, 0)

        def per_expert(e, c):
            q = s * E + e

            @pl.when(q + DEPTH - 1 < S * E)
            def _():
                fetch(q + DEPTH - 1, True)

            fetch(q, False)
            slot_base = lax.rem(q, DEPTH) * seg_rows

            def group(i, cc):
                first = q * CAP + i * 16
                rows = [pl.multiple_of(addr[first + k], 8) for k in range(16)]
                gates = [gate[first + k] for k in range(16)]
                at = [slot_base + (i * 2 + k // 8) * (KB * PITCH) + k % 8 for k in range(16)]
                sums = [acc[a, pl.ds(rows[k], KB), :] + gates[k] * ybuf[pl.ds(at[k], KB, stride=PITCH), :] for k in range(16)]
                for k in range(16):
                    acc[a, pl.ds(rows[k], KB), :] = sums[k]
                return cc

            lax.fori_loop(0, (cnt[q] + 15) // 16, group, 0)
            return c

        lax.fori_loop(0, E, per_expert, 0)
        pltpu.make_async_copy(acc.at[a, pl.ds(0, T * KB)], part.at[s], osem.at[a]).start()
    for s in range(max(S - 2, 0), S):
        pltpu.make_async_copy(acc.at[s % 2, pl.ds(0, T * KB)], part.at[s], osem.at[s % 2]).wait()


def prep_kernel(KB, *refs):
    resid, moe, attn, router = refs[:4]
    u3, nattn, logits, xs = refs[-4:]
    x = resid[0].astype(F32)
    rows = x.shape[0]
    inv = lax.rsqrt(jnp.mean(x * x, axis=-1, keepdims=True) + EPS)
    x = x * inv
    nattn[0] = (x * attn[...].astype(F32)).astype(BF16)
    u = (x * moe[...].astype(F32)).astype(BF16)
    logits[...] = lax.dot_general(router[...], u, (((1,), (1,)), ((), ())), preferred_element_type=F32)
    wide = u.astype(F32)
    for rb in range(rows // 8):
        for k in range(KB):
            xs[pl.ds(rb * 8 * (KB + 1) + k, 8, stride=KB + 1), :] = wide[rb * 8:rb * 8 + 8, k * LANES:(k + 1) * LANES]
    for r in range(rows):
        u3[r] = xs[r * (KB + 1):r * (KB + 1) + KB, :].astype(BF16)


def run_prep(micro, resid, moe, attn, router_t, earlier):
    micros, T, D = resid.shape
    KB = D // LANES
    rows = 128
    experts = router_t.shape[0]
    row_block = pl.BlockSpec((1, rows, D), lambda i: (micro, i, 0))
    scale = pl.BlockSpec((1, D), lambda i: (0, 0))
    args = [resid, moe.reshape(1, D), attn.reshape(1, D), router_t]
    specs = [row_block, scale, scale, pl.BlockSpec((experts, D), lambda i: (0, 0))]
    aliases = {}
    if earlier is not None:
        args.append(earlier)
        specs.append(pl.BlockSpec(memory_space=pl.ANY))
        aliases = {4: 1}
    return pl.pallas_call(
        functools.partial(prep_kernel, KB),
        grid=(T // rows,),
        out_shape=(jax.ShapeDtypeStruct((T, KB, LANES), BF16), jax.ShapeDtypeStruct((micros, T, D), BF16), jax.ShapeDtypeStruct((experts, T), F32)),
        in_specs=specs,
        out_specs=(pl.BlockSpec((rows, KB, LANES), lambda i: (i, 0, 0)), row_block, pl.BlockSpec((experts, rows), lambda i: (0, i))),
        scratch_shapes=[pltpu.VMEM((rows * (KB + 1), LANES), F32)],
        input_output_aliases=aliases,
        compiler_params=pltpu.CompilerParams(vmem_limit_bytes=40_000_000),
        cost_estimate=pl.CostEstimate(flops=3_000_000_000, bytes_accessed=20_000_000, transcendentals=0),
        name='prep',
    )(*args)


def attention_kernel(seq, q_ref, k_ref, v_ref, cos_ref, sin_ref, cos_t, sin_t, o_ref):
    step = 128
    half = LANES // 2
    key = lax.broadcasted_iota(jnp.int32, (step, step), 0)
    query = lax.broadcasted_iota(jnp.int32, (step, step), 1)
    keep = query >= key
    factor = LANES ** -0.5 * 1.4426950408889634
    for hh in range(k_ref.shape[1] // LANES):
        at = hh * LANES
        first, second = q_ref[at:at + half, :], q_ref[at + half:at + LANES, :]
        ct, st = cos_t[...], sin_t[...]
        q = jnp.concatenate([first * ct - second * st, second * ct + first * st], axis=0).astype(BF16)
        kf = k_ref[:, at:at + LANES]
        k = (kf * cos_ref[...] + pltpu.roll(kf, half, 1) * sin_ref[...]).astype(BF16)
        v = v_ref[at:at + LANES, :]
        for j in range(seq // step):
            n = (j + 1) * step
            s = jnp.dot(k[:n], q[:, j * step:n], preferred_element_type=F32)
            diag = jnp.where(keep, s[j * step:], NEG)
            s = jnp.concatenate([s[:j * step], diag], axis=0) if j else diag
            p = jnp.exp2((s - jnp.max(s, axis=0, keepdims=True)) * factor)
            p = (p * (1.0 / jnp.sum(p, axis=0, keepdims=True))).astype(BF16)
            o_ref[at:at + LANES, j * step:n] = jnp.dot(v[:, :n], p, preferred_element_type=F32).astype(BF16)


def run_attention(q_t, k, v_t, seq):
    T, D = k.shape
    half = LANES // 2
    freqs = ROPE_BASE ** (-jnp.arange(half, dtype=F32) * 2.0 / LANES)
    angles = jnp.arange(seq, dtype=F32)[:, None] * freqs[None, :]
    cos_half, sin_half = jnp.cos(angles), jnp.sin(angles)
    cosine = jnp.concatenate([cos_half, cos_half], axis=1)
    sine = jnp.concatenate([-sin_half, sin_half], axis=1)
    block = pl.BlockSpec((seq, 256), lambda i, j: (i, j))
    block_t = pl.BlockSpec((256, seq), lambda i, j: (j, i))
    table = pl.BlockSpec((seq, LANES), lambda i, j: (0, 0))
    table_t = pl.BlockSpec((half, seq), lambda i, j: (0, 0))
    return pl.pallas_call(
        functools.partial(attention_kernel, seq),
        grid=(T // seq, D // 256),
        out_shape=jax.ShapeDtypeStruct((D, T), BF16),
        in_specs=[block_t, block, block_t, table, table, table_t, table_t],
        out_specs=block_t,
        compiler_params=pltpu.CompilerParams(vmem_limit_bytes=40_000_000),
        cost_estimate=pl.CostEstimate(flops=50_000_000_000, bytes_accessed=76_000_000, transcendentals=0),
        name='attention',
    )(q_t, k, v_t, cosine, sine, cos_half.T, sin_half.T)


def final_kernel(KB, b, m, *rest):
    o = rest[-1]
    rows = b.shape[0]
    for k in range(KB):
        cols = slice(k * LANES, (k + 1) * LANES)
        o[0, :, cols] = (b[:, cols] + m[pl.ds(k, rows, stride=KB), :]).astype(BF16)


def run_final(micro, micros, b, m, earlier):
    TT, D = b.shape
    T = TT // micros
    KB = D // LANES
    rows = 256
    per = T // rows
    args = [b, m]
    specs = [pl.BlockSpec((rows, D), lambda i: (micro * per + i, 0)), pl.BlockSpec((rows * KB, LANES), lambda i: (i, 0))]
    aliases = {}
    if earlier is not None:
        args.append(earlier)
        specs.append(pl.BlockSpec(memory_space=pl.ANY))
        aliases = {2: 0}
    return pl.pallas_call(
        functools.partial(final_kernel, KB),
        grid=(per,),
        out_shape=jax.ShapeDtypeStruct((micros, T, D), BF16),
        in_specs=specs,
        out_specs=pl.BlockSpec((1, rows, D), lambda i: (micro, i, 0)),
        input_output_aliases=aliases,
        compiler_params=pltpu.CompilerParams(vmem_limit_bytes=40_000_000),
        cost_estimate=pl.CostEstimate(flops=1_000_000_000, bytes_accessed=32_000_000, transcendentals=0),
        name='final',
    )(*args)


def run_experts(cnt, tok, u, own, other, chips, cap):
    E = 2 * own[0].shape[0]
    D, FE = own[0].shape[1], own[0].shape[2]
    KB = D // LANES
    MAXR = chips * cap
    BIG = 384
    cfg = (E, chips, cap, KB, FE, MAXR, BIG)
    any_spec = pl.BlockSpec(memory_space=pl.ANY)
    smem = pl.BlockSpec(memory_space=pltpu.SMEM)
    flops = chips * cap * E * D * FE * 3
    return pl.pallas_call(
        functools.partial(expert_kernel, cfg),
        out_shape=jax.ShapeDtypeStruct(((E * MAXR + 32) // 8 * KB * PITCH, LANES), F32),
        in_specs=[smem, smem] + [any_spec] * 7,
        out_specs=any_spec,
        scratch_shapes=[
            pltpu.VMEM((2, D, FE), BF16), pltpu.VMEM((2, D, FE), BF16), pltpu.VMEM((2, FE, D), BF16),
            pltpu.VMEM((2 * MAXR, KB, LANES), BF16), pltpu.VMEM((32 * (KB + 1), LANES), F32), pltpu.VMEM((BIG // 16, KB, 16, LANES), BF16),
            pltpu.VMEM((BIG, FE), BF16), pltpu.VMEM((2, BIG // 8 * KB * PITCH, LANES), F32),
            pltpu.SemaphoreType.DMA((2,)), pltpu.SemaphoreType.DMA((2,)), pltpu.SemaphoreType.DMA((2,)),
        ],
        compiler_params=pltpu.CompilerParams(vmem_limit_bytes=66_000_000),
        cost_estimate=pl.CostEstimate(flops=flops, bytes_accessed=400_000_000, transcendentals=0),
        name='experts',
    )(cnt, tok, u, *own, *other)


def run_combine(cnt, pos, addr, gate, y, chips, E, cap, T, KB):
    MAXR = chips * cap
    DEPTH = 4
    cfg = (E, chips, cap, KB, MAXR, T, DEPTH)
    smem = pl.BlockSpec(memory_space=pltpu.SMEM)
    any_spec = pl.BlockSpec(memory_space=pl.ANY)
    return pl.pallas_call(
        functools.partial(combine_kernel, cfg),
        out_shape=jax.ShapeDtypeStruct((chips, T * KB, LANES), F32),
        in_specs=[smem] * 4 + [any_spec],
        out_specs=any_spec,
        scratch_shapes=[
            pltpu.VMEM((2, (T + 8) * KB, LANES), F32), pltpu.VMEM((DEPTH * (cap // 8) * KB * PITCH, LANES), F32),
            pltpu.SemaphoreType.DMA((DEPTH,)), pltpu.SemaphoreType.DMA((2,)),
        ],
        compiler_params=pltpu.CompilerParams(vmem_limit_bytes=66_000_000),
        cost_estimate=pl.CostEstimate(flops=40_000_000_000, bytes_accessed=150_000_000, transcendentals=0),
        name='combine',
    )(cnt, pos, addr, gate, y)


def solution(mesh):
    group_size = mesh.shape['ep']
    tok_spec = P(None, ('dp', 'ep'), None, None)
    rep_one = P(None)
    rep_two = P(None, None)
    rep_three = P(None, None, None)
    expert_spec = P('ep', None, None)
    chips = group_size // 2
    same_core = [[2 * c for c in range(chips)], [2 * c + 1 for c in range(chips)]]
    partner = [(i, i ^ 1) for i in range(group_size)]

    def local_program(resid_in, expert_idx, expert_slot, w_query, w_key, w_value, w_out, w_gate, w_up, w_down, w_router, norm_attn, norm_ffn, norm_moe, expert_gate, expert_up, expert_down):
        micros, seqs, seq_len, width = resid_in.shape
        T = seqs * seq_len
        KB = width // LANES
        choices = expert_idx.shape[-1]
        local_experts = expert_gate.shape[0]
        experts = local_experts * group_size
        E = 2 * local_experts
        cap = CAP_FACTOR * T * choices // experts
        me = lax.axis_index('ep')
        own = (expert_gate, expert_up, expert_down)
        other = tuple(lax.ppermute(w, 'ep', partner) for w in own)

        def mine(table, axis):
            return jnp.concatenate([lax.dynamic_slice_in_dim(table, me * local_experts, local_experts, axis), lax.dynamic_slice_in_dim(table, (me ^ 1) * local_experts, local_experts, axis)], axis)

        resid = resid_in.reshape(micros, T, width)
        router_t = w_router.T
        tokens_all, logits_all, nattn = [], [], None
        for micro in range(micros):
            u3, nattn, logits = run_prep(micro, resid, norm_moe, norm_attn, router_t, nattn)
            tokens_all.append(lax.all_gather(u3, 'ep', axis_index_groups=same_core))
            logits_all.append(logits)
        upper = (jnp.arange(T)[:, None] <= jnp.arange(T)[None, :]).astype(BF16)
        rank_ids = jnp.arange(cap, dtype=F32)[None, :, None]
        expert_ids = jnp.arange(experts)[:, None]
        tables = []
        for micro in range(micros):
            ids = expert_idx[micro].reshape(T, choices).T
            picked = jnp.any(ids[:, None, :] == expert_ids[None], axis=0)
            masked = jnp.where(picked, logits_all[micro], NEG)
            grown = jnp.where(picked, jnp.exp(masked - jnp.max(masked, axis=0, keepdims=True)), 0.0)
            gates = grown / jnp.sum(grown, axis=0, keepdims=True)
            upto = jnp.dot(picked.astype(BF16), upper, preferred_element_type=F32)
            tok_of = jnp.sum((upto[:, None, :] <= rank_ids).astype(F32), axis=-1)
            mark = jnp.where(picked, upto, 0.0)
            gate_of = jnp.sum(jnp.where(mark[:, None, :] == rank_ids + 1.0, gates[:, None, :], 0.0), axis=-1)
            tables.append(mine(lax.all_gather(jnp.concatenate([tok_of, gate_of], axis=-1), 'ep', axis_index_groups=same_core), 1))

        flat = nattn.reshape(micros * T, width)
        across = (((0,), (1,)), ((), ()))
        q_t = lax.dot_general(w_query.reshape(width, -1), flat, across, preferred_element_type=F32)
        k = jnp.dot(flat, w_key.reshape(width, -1), preferred_element_type=F32)
        v_t = lax.dot_general(w_value.reshape(width, -1), flat, across, preferred_element_type=F32).astype(BF16)

        summed = []
        for micro in range(micros):
            tok_of = tables[micro][:, :, :cap].astype(jnp.int32)
            gate_of = tables[micro][:, :, cap:]
            cnt = jnp.sum((tok_of < T).astype(jnp.int32), axis=-1)
            if micro == 0:
                cnt, q_t, k, v_t = lax.optimization_barrier((cnt, q_t, k, v_t))
            padded = (cnt + 7) // 8 * 8
            pos = jnp.cumsum(padded, axis=0) - padded
            row_tok = jnp.minimum(tok_of, T - 1) + jnp.arange(chips, dtype=jnp.int32)[:, None, None] * T
            addr = tok_of * KB
            y = run_experts(cnt.reshape(-1), row_tok.reshape(-1), tokens_all[micro].reshape(chips * T, KB, LANES), own, other, chips, cap)
            part = run_combine(cnt.reshape(-1), pos.reshape(-1), addr.reshape(-1), gate_of.reshape(-1), y, chips, E, cap, T, KB)
            if micro == micros - 1:
                part, q_t, k, v_t = lax.optimization_barrier((part, q_t, k, v_t))
            summed.append(lax.psum_scatter(part, 'ep', scatter_dimension=0, axis_index_groups=same_core))
        o_t = run_attention(q_t, k, v_t, seq_len)
        attn_out = lax.dot_general(o_t, w_out.reshape(-1, width), (((0,), (0,)), ((), ())), preferred_element_type=F32)
        after = (resid.reshape(micros * T, width).astype(F32) + attn_out).astype(BF16)
        dense = ffn_branch(after, norm_ffn, w_gate, w_up, w_down)
        out = None
        for micro in range(micros):
            out = run_final(micro, micros, dense, summed[micro].reshape(T * KB, LANES), out)
        return out.reshape(micros, seqs, seq_len, width)

    return jax.shard_map(local_program, mesh=mesh, in_specs=(tok_spec, tok_spec, tok_spec, rep_three, rep_three, rep_three, rep_three, rep_two, rep_two, rep_two, rep_two, rep_one, rep_one, rep_one, expert_spec, expert_spec, expert_spec), out_specs=tok_spec, check_vma=False)
```

```python
import functools

import jax
import jax.numpy as jnp
from jax import lax
from jax.experimental import pallas as pl
from jax.experimental.pallas import tpu as pltpu
from jax.sharding import PartitionSpec as P

EPS = 1e-6
ROPE_BASE = 10000.0
CAP_FACTOR = 2
NEG = -1e30
LANES = 128
PITCH = 9
F32 = jnp.float32
BF16 = jnp.bfloat16


def rms_norm(values, scale):
    widened = values.astype(F32)
    mean_sq = jnp.mean(widened * widened, axis=-1, keepdims=True)
    return (widened * lax.rsqrt(mean_sq + EPS) * scale.astype(F32)).astype(BF16)


def ffn_branch(after_attn, norm_ffn, w_gate, w_up, w_down):
    normed_ffn = rms_norm(after_attn, norm_ffn)
    gate_act = jnp.dot(normed_ffn, w_gate, preferred_element_type=F32)
    up_act = jnp.dot(normed_ffn, w_up, preferred_element_type=F32)
    hidden = (gate_act * jax.nn.sigmoid(gate_act) * up_act).astype(BF16)
    return after_attn.astype(F32) + jnp.dot(hidden, w_down, preferred_element_type=F32)


def expert_kernel(cfg, cnt, tok, u, wg0, wu0, wd0, wg1, wu1, wd1, y, wg, wu, wd, x3, xs, x2, h, yb, flags, wsem, xsem, ysem):
    E, S, CAP, KB, FE, MAXR, SIZES = cfg
    YROWS = max(SIZES) // 8 * KB * PITCH
    half = E // 2
    D = KB * LANES

    def weights(e, slot, start):
        if not start:
            pltpu.make_async_copy(wg0.at[0], wg.at[slot], wsem.at[slot]).wait()
            pltpu.make_async_copy(wu0.at[0], wu.at[slot], wsem.at[slot]).wait()
            pltpu.make_async_copy(wd0.at[0], wd.at[slot], wsem.at[slot]).wait()
            return

        @pl.when(e < half)
        def _():
            pltpu.make_async_copy(wg0.at[e], wg.at[slot], wsem.at[slot]).start()
            pltpu.make_async_copy(wu0.at[e], wu.at[slot], wsem.at[slot]).start()
            pltpu.make_async_copy(wd0.at[e], wd.at[slot], wsem.at[slot]).start()

        @pl.when(e >= half)
        def _():
            pltpu.make_async_copy(wg1.at[e - half], wg.at[slot], wsem.at[slot]).start()
            pltpu.make_async_copy(wu1.at[e - half], wu.at[slot], wsem.at[slot]).start()
            pltpu.make_async_copy(wd1.at[e - half], wd.at[slot], wsem.at[slot]).start()

    def rows_of(e):
        total = 0
        for s in range(S):
            total = total + (cnt[s * E + e] + 7) // 8
        return total

    def gather(e, slot):
        pos = slot * MAXR
        for s in range(S):
            groups = (cnt[s * E + e] + 7) // 8
            base = (s * E + e) * CAP

            def issue(i, carry, pos=pos, base=base):
                for k in range(8):
                    t = tok[base + i * 8 + k]
                    pltpu.make_async_copy(u.at[t], x3.at[pos + i * 8 + k], xsem.at[slot]).start()
                return carry

            lax.fori_loop(0, groups, issue, 0)
            pos = pos + groups * 8

    def gather_wait(e, slot):
        def one(i, carry):
            pltpu.make_async_copy(u.at[pl.ds(0, 8)], x3.at[pl.ds(0, 8)], xsem.at[slot]).wait()
            return carry

        lax.fori_loop(0, rows_of(e), one, 0)

    def y_copy(rows, par, dst):
        n = rows // 8 * KB * PITCH
        return pltpu.make_async_copy(yb.at[pl.ds(pl.multiple_of(par * YROWS, 8), n)], y.at[pl.ds(dst, n)], ysem.at[par])

    def y_drain(par):
        for which, rows in enumerate(SIZES):
            @pl.when(flags[par] == which + 1)
            def _(rows=rows):
                y_copy(rows, par, 0).wait()

    def block(e, slot, r0, M):
        src = slot * MAXR + r0
        par = flags[2]
        y_drain(par)
        flags[par] = SIZES.index(M) + 1
        flags[2] = 1 - par
        ybase = par * YROWS

        def relayout(g, carry):
            for i in range(32):
                xs[i * (KB + 1):i * (KB + 1) + KB, :] = x3[src + g * 32 + i].astype(F32)
            for half in range(2):
                for k in range(KB):
                    x2[g * 2 + half, k] = xs[pl.ds(half * 16 * (KB + 1) + k, 16, stride=KB + 1), :].astype(BF16)
            return carry

        lax.fori_loop(0, M // 32, relayout, 0)
        x = jnp.concatenate([x2[0:M // 16, k].reshape(M, LANES) for k in range(KB)], axis=1)
        full = FE // 256
        for j in range(full):
            cols = slice(j * 256, j * 256 + 256)
            ga = jnp.dot(x, wg[slot, :, cols], preferred_element_type=F32)
            ua = jnp.dot(x, wu[slot, :, cols], preferred_element_type=F32)
            h[0:M, cols] = (ga * jax.nn.sigmoid(ga) * ua).astype(BF16)
        if FE % 256:
            cols = slice(full * 256, FE)
            width = FE - full * 256
            both = jnp.dot(x, jnp.concatenate([wg[slot, :, cols], wu[slot, :, cols]], axis=1), preferred_element_type=F32)
            ga, ua = both[:, :width], both[:, width:]
            h[0:M, cols] = (ga * jax.nn.sigmoid(ga) * ua).astype(BF16)
        hid = h[0:M, :]
        for j in range(D // 256):
            out = jnp.dot(hid, wd[slot, :, j * 256:j * 256 + 256], preferred_element_type=F32)
            out = out.astype(BF16).astype(F32)
            for rb in range(M // 8):
                for k in range(2):
                    at = (rb * KB + 2 * j + k) * PITCH
                    yb[pl.ds(ybase + at, 8), :] = out[rb * 8:rb * 8 + 8, k * LANES:(k + 1) * LANES]
        dst = pl.multiple_of((e * MAXR + r0) // 8 * (KB * PITCH), 8)
        y_copy(M, par, dst).start()

    flags[0] = 0
    flags[1] = 0
    flags[2] = 0
    weights(0, 0, True)
    gather(0, 0)

    def per_expert(e, carry):
        slot = lax.rem(e, 2)
        weights(e, slot, False)
        gather_wait(e, slot)

        @pl.when(e + 1 < E)
        def _():
            weights(e + 1, 1 - slot, True)
            gather(e + 1, 1 - slot)

        units = (rows_of(e) + 7) // 8
        count = jnp.where(units == 7, 2, units // 4)
        rest = jnp.where(units == 7, 0, lax.rem(units, 4))
        rest = jnp.where(units < 4, 0, rest)
        count = jnp.where(jnp.logical_and(units > 0, units < 4), 1, count)
        large = (rest >= 2).astype(jnp.int32)
        medium = lax.rem(rest, 2)

        @pl.when(large == 1)
        def _():
            block(e, slot, 0, 384)

        @pl.when(medium == 1)
        def _():
            block(e, slot, pl.multiple_of(large * 384, 64), 320)

        def plain(i, c):
            block(e, slot, pl.multiple_of(large * 384 + medium * 320 + i * 256, 64), 256)
            return c

        lax.fori_loop(0, count - large - medium, plain, 0)
        return carry

    lax.fori_loop(0, E, per_expert, 0)
    for par in range(2):
        y_drain(par)


def combine_kernel(cfg, cnt, pos, addr, gate, y, part, acc, ybuf, ysem, osem):
    E, S, CAP, KB, MAXR, T, DEPTH = cfg
    PIECE = 32
    seg_rows = CAP // 8 * KB * PITCH
    piece_rows = PIECE // 8 * KB * PITCH

    def fetch(q, start):
        slot = lax.rem(q, DEPTH)
        s = q // E
        e = q - s * E
        pieces = (cnt[q] + PIECE - 1) // PIECE
        base = pl.multiple_of((e * MAXR + pos[q]) // 8 * (KB * PITCH), 8)

        def one(i, c):
            src = y.at[pl.ds(pl.multiple_of(base + i * piece_rows, 8), piece_rows)]
            dst = ybuf.at[pl.ds(pl.multiple_of(slot * seg_rows + i * piece_rows, 8), piece_rows)]
            copy = pltpu.make_async_copy(src, dst, ysem.at[slot])
            copy.start() if start else copy.wait()
            return c

        lax.fori_loop(0, pieces, one, 0)

    for q in range(DEPTH - 1):
        fetch(q, True)
    zero = jnp.zeros((8 * KB, LANES), F32)
    for s in range(S):
        a = s % 2
        if s >= 2:
            pltpu.make_async_copy(acc.at[a, pl.ds(0, T * KB)], part.at[s - 2], osem.at[a]).wait()

        def clear(i, c):
            acc[a, pl.ds(pl.multiple_of(i * 8 * KB, 8), 8 * KB), :] = zero
            return c

        lax.fori_loop(0, T // 8, clear, 0)

        def per_expert(e, c):
            q = s * E + e

            @pl.when(q + DEPTH - 1 < S * E)
            def _():
                fetch(q + DEPTH - 1, True)

            fetch(q, False)
            slot_base = lax.rem(q, DEPTH) * seg_rows

            def group(i, cc):
                first = q * CAP + i * 16
                rows = [pl.multiple_of(addr[first + k], 8) for k in range(16)]
                gates = [gate[first + k] for k in range(16)]
                at = [slot_base + (i * 2 + k // 8) * (KB * PITCH) + k % 8 for k in range(16)]
                sums = [acc[a, pl.ds(rows[k], KB), :] + gates[k] * ybuf[pl.ds(at[k], KB, stride=PITCH), :] for k in range(16)]
                for k in range(16):
                    acc[a, pl.ds(rows[k], KB), :] = sums[k]
                return cc

            lax.fori_loop(0, (cnt[q] + 15) // 16, group, 0)
            return c

        lax.fori_loop(0, E, per_expert, 0)
        pltpu.make_async_copy(acc.at[a, pl.ds(0, T * KB)], part.at[s], osem.at[a]).start()
    for s in range(max(S - 2, 0), S):
        pltpu.make_async_copy(acc.at[s % 2, pl.ds(0, T * KB)], part.at[s], osem.at[s % 2]).wait()


def prep_kernel(KB, *refs):
    resid, moe, attn, router = refs[:4]
    u3, nattn, logits, xs = refs[-4:]
    x = resid[0].astype(F32)
    rows = x.shape[0]
    inv = lax.rsqrt(jnp.mean(x * x, axis=-1, keepdims=True) + EPS)
    x = x * inv
    nattn[0] = (x * attn[...].astype(F32)).astype(BF16)
    u = (x * moe[...].astype(F32)).astype(BF16)
    logits[0] = lax.dot_general(router[...], u, (((1,), (1,)), ((), ())), preferred_element_type=F32)
    wide = u.astype(F32)
    for rb in range(rows // 8):
        for k in range(KB):
            xs[pl.ds(rb * 8 * (KB + 1) + k, 8, stride=KB + 1), :] = wide[rb * 8:rb * 8 + 8, k * LANES:(k + 1) * LANES]
    for r in range(rows):
        u3[r] = xs[r * (KB + 1):r * (KB + 1) + KB, :].astype(BF16)


def run_prep(micro, resid, moe, attn, router_t, earlier):
    micros, T, D = resid.shape
    KB = D // LANES
    rows = min(256, T)
    experts = router_t.shape[0]
    row_block = pl.BlockSpec((1, rows, D), lambda i: (micro, i, 0))
    scale = pl.BlockSpec((1, D), lambda i: (0, 0))
    args = [resid, moe.reshape(1, D), attn.reshape(1, D), router_t]
    specs = [row_block, scale, scale, pl.BlockSpec((experts, D), lambda i: (0, 0))]
    aliases = {}
    if earlier is not None:
        args += list(earlier)
        specs += [pl.BlockSpec(memory_space=pl.ANY)] * 2
        aliases = {4: 1, 5: 2}
    return pl.pallas_call(
        functools.partial(prep_kernel, KB),
        grid=(T // rows,),
        out_shape=(jax.ShapeDtypeStruct((T, KB, LANES), BF16), jax.ShapeDtypeStruct((micros, T, D), BF16), jax.ShapeDtypeStruct((micros, experts, T), F32)),
        in_specs=specs,
        out_specs=(pl.BlockSpec((rows, KB, LANES), lambda i: (i, 0, 0)), row_block, pl.BlockSpec((1, experts, rows), lambda i: (micro, 0, i))),
        scratch_shapes=[pltpu.VMEM((rows * (KB + 1), LANES), F32)],
        input_output_aliases=aliases,
        compiler_params=pltpu.CompilerParams(vmem_limit_bytes=66_000_000),
        cost_estimate=pl.CostEstimate(flops=3_000_000_000, bytes_accessed=20_000_000, transcendentals=0),
        name='prep',
    )(*args)


def route_kernel(cfg, ids, logits, table, marks, highs, mids, lows, begins, owners):
    E, T, CAP, NB, SP = cfg
    experts = lax.broadcasted_iota(jnp.int32, (E, T), 0)
    picked = ids[0, 0:1, :] == experts
    for j in range(1, ids.shape[1]):
        picked = jnp.logical_or(picked, ids[0, j:j + 1, :] == experts)
    masked = jnp.where(picked, logits[0], NEG)
    grown = jnp.where(picked, jnp.exp(masked - jnp.max(masked, axis=0, keepdims=True)), 0.0)
    gates = grown / jnp.sum(grown, axis=0, keepdims=True)
    flags = picked.astype(F32)
    row = lax.broadcasted_iota(jnp.int32, (LANES, LANES), 0)
    col = lax.broadcasted_iota(jnp.int32, (LANES, LANES), 1)
    tri = (row <= col).astype(F32).astype(BF16)
    lane48 = lax.broadcasted_iota(jnp.int32, (E, LANES), 1)
    start = jnp.zeros((E, 1), F32)
    starts = jnp.zeros((E, LANES), F32)
    ends = jnp.zeros((E, LANES), F32)
    for ref in (marks, highs, mids, lows, begins, owners):
        ref[...] = jnp.zeros(ref.shape, F32)
    for b in range(NB):
        cols = slice(b * LANES, (b + 1) * LANES)
        f = flags[:, cols]
        upto = jnp.dot(f.astype(BF16), tri, preferred_element_type=F32)
        g = gates[:, cols]
        high = g.astype(BF16).astype(F32)
        mid = (g - high).astype(BF16).astype(F32)
        low = g - high - mid
        at = slice(b * SP, b * SP + E)
        marks[at, :] = f * upto
        highs[at, :] = high
        mids[at, :] = mid
        lows[at, :] = low
        begins[at, :] = jnp.broadcast_to(start, (E, LANES))
        owners[at, :] = jnp.full((E, LANES), float(b), F32)
        end = start + upto[:, LANES - 1:LANES]
        here = lane48 % 16 == b
        starts = jnp.where(here, start, starts)
        ends = jnp.where(here, end, ends)
        start = end
    rank = lax.broadcasted_iota(jnp.int32, (CAP, LANES), 0).astype(F32)
    lane = lax.broadcasted_iota(jnp.int32, (CAP, LANES), 1)
    lane_f = lane.astype(F32)
    total = start
    out = jnp.zeros((CAP, LANES), F32)
    for e in range(E):
        def rows_at(ref):
            return ref[pl.ds(e, 16, stride=SP), :]
        begin = rows_at(begins)
        over = jnp.where(begin >= 256.0, 256.0, 0.0)
        zero = jnp.zeros((16, 4 * LANES), F32)
        first = jnp.concatenate([rows_at(marks), rows_at(highs), rows_at(mids), rows_at(lows), rows_at(owners)], axis=1)
        second = jnp.concatenate([begin - over, zero], axis=1)
        third = jnp.concatenate([over, zero], axis=1)
        grid = jnp.concatenate([first, second, third, jnp.zeros((LANES - 48, 5 * LANES), F32)], axis=0).astype(BF16)
        mine = jnp.logical_and(rank >= starts[e:e + 1], rank < ends[e:e + 1])
        hot = jnp.where(jnp.logical_and(mine, lane < 48), 1.0, 0.0).astype(BF16)
        got = jnp.dot(hot, grid, preferred_element_type=F32)
        same = got[:, :LANES] == rank + 1.0
        gate = jnp.where(same, got[:, LANES:2 * LANES] + got[:, 2 * LANES:3 * LANES] + got[:, 3 * LANES:4 * LANES], 0.0)
        token = jnp.where(same, lane_f + float(LANES) * got[:, 4 * LANES:], 0.0)
        gate = jnp.sum(gate, axis=1, keepdims=True)
        token = jnp.sum(token, axis=1, keepdims=True)
        token = jnp.where(rank[:, :1] < total[e:e + 1], token, float(T))
        out = jnp.where(lane == e, token, out)
        out = jnp.where(lane == LANES // 2 + e, gate, out)
    pad = jnp.zeros((table.shape[2] - CAP, LANES), F32)
    table[0] = jnp.concatenate([out, pad], axis=0).T


def run_route(ids, logits, cap):
    micros, E, T = logits.shape
    NB = T // LANES
    SP = E + 1 if E % 8 == 0 else E
    wide = -(-cap // LANES) * LANES
    rows = 16 * SP
    return pl.pallas_call(
        functools.partial(route_kernel, (E, T, cap, NB, SP)),
        grid=(micros,),
        out_shape=jax.ShapeDtypeStruct((micros, LANES, wide), F32),
        in_specs=[pl.BlockSpec((1,) + ids.shape[1:], lambda i: (i, 0, 0)), pl.BlockSpec((1, E, T), lambda i: (i, 0, 0))],
        out_specs=pl.BlockSpec((1, LANES, wide), lambda i: (i, 0, 0)),
        scratch_shapes=[pltpu.VMEM((rows, LANES), F32)] * 6,
        compiler_params=pltpu.CompilerParams(vmem_limit_bytes=40_000_000),
        cost_estimate=pl.CostEstimate(flops=20_000_000_000, bytes_accessed=2_000_000, transcendentals=0),
        name='route',
    )(ids, logits)


def attention_kernel(seq, q_ref, k_ref, v_ref, cos_ref, sin_ref, cos_t, sin_t, o_ref):
    step = 128
    half = LANES // 2
    key = lax.broadcasted_iota(jnp.int32, (step, step), 0)
    query = lax.broadcasted_iota(jnp.int32, (step, step), 1)
    keep = query >= key
    factor = LANES ** -0.5 * 1.4426950408889634
    for hh in range(k_ref.shape[1] // LANES):
        at = hh * LANES
        first, second = q_ref[at:at + half, :], q_ref[at + half:at + LANES, :]
        ct, st = cos_t[...], sin_t[...]
        q = jnp.concatenate([first * ct - second * st, second * ct + first * st], axis=0).astype(BF16)
        kf = k_ref[:, at:at + LANES]
        k = (kf * cos_ref[...] + pltpu.roll(kf, half, 1) * sin_ref[...]).astype(BF16)
        v = v_ref[at:at + LANES, :]
        for j in range(seq // step):
            n = (j + 1) * step
            s = jnp.dot(k[:n], q[:, j * step:n], preferred_element_type=F32)
            diag = jnp.where(keep, s[j * step:], NEG)
            s = jnp.concatenate([s[:j * step], diag], axis=0) if j else diag
            p = jnp.exp2((s - jnp.max(s, axis=0, keepdims=True)) * factor)
            p = (p * (1.0 / jnp.sum(p, axis=0, keepdims=True))).astype(BF16)
            o_ref[at:at + LANES, j * step:n] = jnp.dot(v[:, :n], p, preferred_element_type=F32).astype(BF16)


def run_attention(q_t, k, v_t, seq):
    T, D = k.shape
    half = LANES // 2
    freqs = ROPE_BASE ** (-jnp.arange(half, dtype=F32) * 2.0 / LANES)
    angles = jnp.arange(seq, dtype=F32)[:, None] * freqs[None, :]
    cos_half, sin_half = jnp.cos(angles), jnp.sin(angles)
    cosine = jnp.concatenate([cos_half, cos_half], axis=1)
    sine = jnp.concatenate([-sin_half, sin_half], axis=1)
    wide = min(D, 512)
    block = pl.BlockSpec((seq, wide), lambda i, j: (i, j))
    block_t = pl.BlockSpec((wide, seq), lambda i, j: (j, i))
    table = pl.BlockSpec((seq, LANES), lambda i, j: (0, 0))
    table_t = pl.BlockSpec((half, seq), lambda i, j: (0, 0))
    return pl.pallas_call(
        functools.partial(attention_kernel, seq),
        grid=(T // seq, D // wide),
        out_shape=jax.ShapeDtypeStruct((D, T), BF16),
        in_specs=[block_t, block, block_t, table, table, table_t, table_t],
        out_specs=block_t,
        compiler_params=pltpu.CompilerParams(vmem_limit_bytes=40_000_000),
        cost_estimate=pl.CostEstimate(flops=50_000_000_000, bytes_accessed=76_000_000, transcendentals=0),
        name='attention',
    )(q_t, k, v_t, cosine, sine, cos_half.T, sin_half.T)


def final_kernel(KB, b, m, *rest):
    o = rest[-1]
    rows = b.shape[0]
    for k in range(KB):
        cols = slice(k * LANES, (k + 1) * LANES)
        o[0, :, cols] = (b[:, cols] + m[pl.ds(k, rows, stride=KB), :]).astype(BF16)


def run_final(micro, micros, b, m, earlier):
    TT, D = b.shape
    T = TT // micros
    KB = D // LANES
    rows = 256
    per = T // rows
    args = [b, m]
    specs = [pl.BlockSpec((rows, D), lambda i: (micro * per + i, 0)), pl.BlockSpec((rows * KB, LANES), lambda i: (i, 0))]
    aliases = {}
    if earlier is not None:
        args.append(earlier)
        specs.append(pl.BlockSpec(memory_space=pl.ANY))
        aliases = {2: 0}
    return pl.pallas_call(
        functools.partial(final_kernel, KB),
        grid=(per,),
        out_shape=jax.ShapeDtypeStruct((micros, T, D), BF16),
        in_specs=specs,
        out_specs=pl.BlockSpec((1, rows, D), lambda i: (micro, i, 0)),
        input_output_aliases=aliases,
        compiler_params=pltpu.CompilerParams(vmem_limit_bytes=66_000_000),
        cost_estimate=pl.CostEstimate(flops=1_000_000_000, bytes_accessed=32_000_000, transcendentals=0),
        name='final',
    )(*args)


def run_experts(cnt, tok, u, own, other, chips, cap):
    E = 2 * own[0].shape[0]
    D, FE = own[0].shape[1], own[0].shape[2]
    KB = D // LANES
    MAXR = chips * cap
    BIG = 384
    cfg = (E, chips, cap, KB, FE, MAXR, (256, 320, 384))
    any_spec = pl.BlockSpec(memory_space=pl.ANY)
    smem = pl.BlockSpec(memory_space=pltpu.SMEM)
    flops = chips * cap * E * D * FE * 3
    return pl.pallas_call(
        functools.partial(expert_kernel, cfg),
        out_shape=jax.ShapeDtypeStruct(((E * MAXR + 32) // 8 * KB * PITCH, LANES), F32),
        in_specs=[smem, smem] + [any_spec] * 7,
        out_specs=any_spec,
        scratch_shapes=[
            pltpu.VMEM((2, D, FE), BF16), pltpu.VMEM((2, D, FE), BF16), pltpu.VMEM((2, FE, D), BF16),
            pltpu.VMEM((2 * MAXR, KB, LANES), BF16), pltpu.VMEM((32 * (KB + 1), LANES), F32), pltpu.VMEM((BIG // 16, KB, 16, LANES), BF16),
            pltpu.VMEM((BIG, FE), BF16), pltpu.VMEM((2 * BIG // 8 * KB * PITCH, LANES), F32), pltpu.SMEM((3,), jnp.int32),
            pltpu.SemaphoreType.DMA((2,)), pltpu.SemaphoreType.DMA((2,)), pltpu.SemaphoreType.DMA((2,)),
        ],
        compiler_params=pltpu.CompilerParams(vmem_limit_bytes=66_000_000),
        cost_estimate=pl.CostEstimate(flops=flops, bytes_accessed=400_000_000, transcendentals=0),
        name='experts',
    )(cnt, tok, u, *own, *other)


def run_combine(cnt, pos, addr, gate, y, chips, E, cap, T, KB):
    MAXR = chips * cap
    DEPTH = 4
    cfg = (E, chips, cap, KB, MAXR, T, DEPTH)
    smem = pl.BlockSpec(memory_space=pltpu.SMEM)
    any_spec = pl.BlockSpec(memory_space=pl.ANY)
    return pl.pallas_call(
        functools.partial(combine_kernel, cfg),
        out_shape=jax.ShapeDtypeStruct((chips, T * KB, LANES), F32),
        in_specs=[smem] * 4 + [any_spec],
        out_specs=any_spec,
        scratch_shapes=[
            pltpu.VMEM((2, (T + 8) * KB, LANES), F32), pltpu.VMEM((DEPTH * (cap // 8) * KB * PITCH, LANES), F32),
            pltpu.SemaphoreType.DMA((DEPTH,)), pltpu.SemaphoreType.DMA((2,)),
        ],
        compiler_params=pltpu.CompilerParams(vmem_limit_bytes=66_000_000),
        cost_estimate=pl.CostEstimate(flops=40_000_000_000, bytes_accessed=150_000_000, transcendentals=0),
        name='combine',
    )(cnt, pos, addr, gate, y)


def solution(mesh):
    group_size = mesh.shape['ep']
    tok_spec = P(None, ('dp', 'ep'), None, None)
    rep_one = P(None)
    rep_two = P(None, None)
    rep_three = P(None, None, None)
    expert_spec = P('ep', None, None)
    chips = group_size // 2
    same_core = [[2 * c for c in range(chips)], [2 * c + 1 for c in range(chips)]]
    partner = [(i, i ^ 1) for i in range(group_size)]

    def local_program(resid_in, expert_idx, expert_slot, w_query, w_key, w_value, w_out, w_gate, w_up, w_down, w_router, norm_attn, norm_ffn, norm_moe, expert_gate, expert_up, expert_down):
        micros, seqs, seq_len, width = resid_in.shape
        T = seqs * seq_len
        KB = width // LANES
        choices = expert_idx.shape[-1]
        local_experts = expert_gate.shape[0]
        experts = local_experts * group_size
        E = 2 * local_experts
        cap = CAP_FACTOR * T * choices // experts
        me = lax.axis_index('ep')
        own = (expert_gate, expert_up, expert_down)
        other = tuple(lax.ppermute(w, 'ep', partner) for w in own)

        resid = resid_in.reshape(micros, T, width)
        router_t = w_router.T
        tokens_all, nattn, logits = [], None, None
        for micro in range(micros):
            u3, nattn, logits = run_prep(micro, resid, norm_moe, norm_attn, router_t, (nattn, logits) if micro else None)
            tokens_all.append(lax.all_gather(u3, 'ep', axis_index_groups=same_core))
        ids = expert_idx.reshape(micros, T, choices).transpose(0, 2, 1)
        table = run_route(ids, logits, cap)
        table = table.reshape(micros, 2, LANES // 2, -1)[:, :, :experts].reshape(micros, 2, chips, E, -1)
        table = lax.all_to_all(table, 'ep', 2, 2, tiled=True, axis_index_groups=same_core)
        core = lax.rem(me, 2)
        table = jnp.concatenate([lax.dynamic_slice_in_dim(table, core * local_experts, local_experts, 3), lax.dynamic_slice_in_dim(table, (1 - core) * local_experts, local_experts, 3)], 3)

        flat = nattn.reshape(micros * T, width)
        across = (((0,), (1,)), ((), ()))
        q_t = lax.dot_general(w_query.reshape(width, -1), flat, across, preferred_element_type=F32)
        k = jnp.dot(flat, w_key.reshape(width, -1), preferred_element_type=F32)
        v_t = lax.dot_general(w_value.reshape(width, -1), flat, across, preferred_element_type=F32).astype(BF16)
        o_t = run_attention(q_t, k, v_t, seq_len)

        summed = []
        for micro in range(micros):
            tok_of = table[micro, 0, :, :, :cap].astype(jnp.int32)
            gate_of = table[micro, 1, :, :, :cap]
            cnt = jnp.sum((tok_of < T).astype(jnp.int32), axis=-1)
            if micro == 0:
                cnt, o_t = lax.optimization_barrier((cnt, o_t))
            padded = (cnt + 7) // 8 * 8
            pos = jnp.cumsum(padded, axis=0) - padded
            row_tok = jnp.minimum(tok_of, T - 1) + jnp.arange(chips, dtype=jnp.int32)[:, None, None] * T
            addr = tok_of * KB
            y = run_experts(cnt.reshape(-1), row_tok.reshape(-1), tokens_all[micro].reshape(chips * T, KB, LANES), own, other, chips, cap)
            part = run_combine(cnt.reshape(-1), pos.reshape(-1), addr.reshape(-1), gate_of.reshape(-1), y, chips, E, cap, T, KB)
            if micro == micros - 1:
                part, o_t = lax.optimization_barrier((part, o_t))
            summed.append(lax.psum_scatter(part, 'ep', scatter_dimension=0, axis_index_groups=same_core))
        attn_out = lax.dot_general(o_t, w_out.reshape(-1, width), (((0,), (0,)), ((), ())), preferred_element_type=F32)
        after = (resid.reshape(micros * T, width).astype(F32) + attn_out).astype(BF16)
        dense = ffn_branch(after, norm_ffn, w_gate, w_up, w_down)
        out = None
        for micro in range(micros):
            out = run_final(micro, micros, dense, summed[micro].reshape(T * KB, LANES), out)
        return out.reshape(micros, seqs, seq_len, width)

    return jax.shard_map(local_program, mesh=mesh, in_specs=(tok_spec, tok_spec, tok_spec, rep_three, rep_three, rep_three, rep_three, rep_two, rep_two, rep_two, rep_two, rep_one, rep_one, rep_one, expert_spec, expert_spec, expert_spec), out_specs=tok_spec, check_vma=False)
```

```python
import functools

import jax
import jax.numpy as jnp
from jax import lax
from jax.experimental import pallas as pl
from jax.experimental.pallas import tpu as pltpu
from jax.sharding import PartitionSpec as P

EPS = 1e-6
ROPE_BASE = 10000.0
CAP_FACTOR = 2
NEG = -1e30
LANES = 128
PITCH = 9
FIRST_SHARE = 0.42
F32 = jnp.float32
BF16 = jnp.bfloat16


def rms_norm(values, scale):
    widened = values.astype(F32)
    mean_sq = jnp.mean(widened * widened, axis=-1, keepdims=True)
    return (widened * lax.rsqrt(mean_sq + EPS) * scale.astype(F32)).astype(BF16)


def ffn_branch(after_attn, norm_ffn, w_gate, w_up, w_down):
    normed_ffn = rms_norm(after_attn, norm_ffn)
    gate_act = jnp.dot(normed_ffn, w_gate, preferred_element_type=F32)
    up_act = jnp.dot(normed_ffn, w_up, preferred_element_type=F32)
    hidden = (gate_act * jax.nn.sigmoid(gate_act) * up_act).astype(BF16)
    return after_attn.astype(F32) + jnp.dot(hidden, w_down, preferred_element_type=F32)


def expert_kernel(cfg, meta, lst, gcol, u, wg0, wu0, wd0, wg1, wu1, wd1, y, wg, wu, wd, gb, x3, xs, x2, h, yb, flags, plan, wsem, xsem, ysem):
    E, KB, FE, MAXR, WIDE, LIMIT, SIZES = cfg
    ENTRIES = plan.shape[0] // 3
    YROWS = max(SIZES) // 8 * KB * PITCH
    half = E // 2
    D = KB * LANES

    def expert_of(v):
        return plan[v]

    def first_of(v):
        return plan[ENTRIES + v]

    def groups_of(v):
        return plan[2 * ENTRIES + v]

    def weights(v, slot, start):
        if not start:
            pltpu.make_async_copy(wg0.at[0], wg.at[slot], wsem.at[slot]).wait()
            pltpu.make_async_copy(wu0.at[0], wu.at[slot], wsem.at[slot]).wait()
            pltpu.make_async_copy(wd0.at[0], wd.at[slot], wsem.at[slot]).wait()
            pltpu.make_async_copy(gcol.at[0, pl.ds(0, LIMIT)], gb.at[pl.ds(0, LIMIT)], wsem.at[slot]).wait()
            return

        e = expert_of(v)
        first = pl.multiple_of(first_of(v), 8)
        pltpu.make_async_copy(gcol.at[e, pl.ds(first, LIMIT)], gb.at[pl.ds(pl.multiple_of(slot * LIMIT, 8), LIMIT)], wsem.at[slot]).start()

        @pl.when(e < half)
        def _():
            pltpu.make_async_copy(wg0.at[e], wg.at[slot], wsem.at[slot]).start()
            pltpu.make_async_copy(wu0.at[e], wu.at[slot], wsem.at[slot]).start()
            pltpu.make_async_copy(wd0.at[e], wd.at[slot], wsem.at[slot]).start()

        @pl.when(e >= half)
        def _():
            pltpu.make_async_copy(wg1.at[e - half], wg.at[slot], wsem.at[slot]).start()
            pltpu.make_async_copy(wu1.at[e - half], wu.at[slot], wsem.at[slot]).start()
            pltpu.make_async_copy(wd1.at[e - half], wd.at[slot], wsem.at[slot]).start()

    def issue_row(base, slot, r):
        pltpu.make_async_copy(u.at[lst[base + r]], x3.at[slot * LIMIT + r], xsem.at[slot]).start()

    def gather(v, slot, begin):
        base = expert_of(v) * WIDE + first_of(v)

        def issue(i, carry):
            for k in range(8):
                issue_row(base, slot, i * 8 + k)
            return carry

        lax.fori_loop(begin, groups_of(v), issue, 0)

    def gather_wait(slot, groups):
        for rows in (64, 8):
            def one(i, carry, rows=rows):
                pltpu.make_async_copy(u.at[pl.ds(0, rows)], x3.at[pl.ds(0, rows)], xsem.at[slot]).wait()
                return carry

            lax.fori_loop(0, groups // 8 if rows == 64 else lax.rem(groups, 8), one, 0)

    def y_copy(rows, par, dst):
        n = rows // 8 * KB * PITCH
        return pltpu.make_async_copy(yb.at[pl.ds(pl.multiple_of(par * YROWS, 8), n)], y.at[pl.ds(dst, n)], ysem.at[par])

    def y_drain(par):
        for which, rows in enumerate(SIZES):
            @pl.when(flags[par] == which + 1)
            def _(rows=rows):
                y_copy(rows, par, 0).wait()

    def block(v, slot, r0, M):
        src = slot * LIMIT + r0
        par = flags[2]
        y_drain(par)
        flags[par] = SIZES.index(M) + 1
        flags[2] = 1 - par
        ybase = par * YROWS
        issued = flags[3]
        flags[3] = issued + M
        gbase = slot * LIMIT + r0
        base = expert_of(v + 1) * WIDE + first_of(v + 1) + issued
        steps = -(-FE // 256) + D // 256

        def ahead(step):
            for r in range(M * step // steps, M * (step + 1) // steps):
                pltpu.make_async_copy(u.at[lst[base + r]], x3.at[(1 - slot) * LIMIT + issued + r], xsem.at[1 - slot]).start()


        def relayout(g, carry):
            for i in range(32):
                xs[i * (KB + 1):i * (KB + 1) + KB, :] = x3[src + g * 32 + i].astype(F32)
            for half in range(2):
                for k in range(KB):
                    x2[g * 2 + half, k] = xs[pl.ds(half * 16 * (KB + 1) + k, 16, stride=KB + 1), :].astype(BF16)
            return carry

        lax.fori_loop(0, M // 32, relayout, 0)
        x = jnp.concatenate([x2[0:M // 16, k].reshape(M, LANES) for k in range(KB)], axis=1)
        full = FE // 256
        for j in range(full):
            cols = slice(j * 256, j * 256 + 256)
            ga = jnp.dot(x, wg[slot, :, cols], preferred_element_type=F32)
            ua = jnp.dot(x, wu[slot, :, cols], preferred_element_type=F32)
            h[0:M, cols] = (ga * jax.nn.sigmoid(ga) * ua).astype(BF16)
            ahead(j)
        if FE % 256:
            ahead(full)
            cols = slice(full * 256, FE)
            width = FE - full * 256
            both = jnp.dot(x, jnp.concatenate([wg[slot, :, cols], wu[slot, :, cols]], axis=1), preferred_element_type=F32)
            ga, ua = both[:, :width], both[:, width:]
            h[0:M, cols] = (ga * jax.nn.sigmoid(ga) * ua).astype(BF16)
        hid = h[0:M, :]
        for j in range(D // 256):
            out = jnp.dot(hid, wd[slot, :, j * 256:j * 256 + 256], preferred_element_type=F32)
            out = out.astype(BF16).astype(F32)
            ahead(steps - D // 256 + j)
            for rb in range(M // 8):
                weight = gb[pl.ds(pl.multiple_of(gbase + rb * 8, 8), 8), :]
                for k in range(2):
                    at = (rb * KB + 2 * j + k) * PITCH
                    yb[pl.ds(ybase + at, 8), :] = weight * out[rb * 8:rb * 8 + 8, k * LANES:(k + 1) * LANES]
        dst = pl.multiple_of((expert_of(v) * MAXR + first_of(v) + r0) // 8 * (KB * PITCH), 8)
        y_copy(M, par, dst).start()

    flags[0] = 0
    flags[1] = 0
    flags[2] = 0
    def blank(i, carry):
        plan[i] = 0
        return carry

    lax.fori_loop(0, 3 * ENTRIES, blank, 0)

    def add(e, at):
        groups = meta[e * LANES + 8] // 8
        for part in range(-(-MAXR // LIMIT)):
            take = jnp.clip(groups - part * (LIMIT // 8), 0, LIMIT // 8)

            @pl.when(take > 0)
            def _(part=part, take=take, at=at):
                plan[at] = e
                plan[ENTRIES + at] = part * LIMIT
                plan[2 * ENTRIES + at] = take

            at = at + (take > 0).astype(jnp.int32)
        return at

    entries = jnp.maximum(lax.fori_loop(0, E, add, jnp.int32(0)), 1)
    weights(0, 0, True)
    gather(0, 0, 0)
    flags[4] = groups_of(0)

    def per_expert(e, carry):
        slot = lax.rem(e, 2)
        weights(e, slot, False)
        gather_wait(slot, flags[4])
        flags[3] = 0

        @pl.when(e + 1 < entries)
        def _():
            weights(e + 1, 1 - slot, True)

        units = (groups_of(e) + 7) // 8
        count = jnp.where(units == 7, 2, units // 4)
        rest = jnp.where(units == 7, 0, lax.rem(units, 4))
        rest = jnp.where(units < 4, 0, rest)
        count = jnp.where(jnp.logical_and(units > 0, units < 4), 1, count)
        large = (rest >= 2).astype(jnp.int32)
        medium = lax.rem(rest, 2)

        @pl.when(large == 1)
        def _():
            block(e, slot, 0, 384)

        @pl.when(medium == 1)
        def _():
            block(e, slot, pl.multiple_of(large * 384, 64), 320)

        def plain(i, c):
            block(e, slot, pl.multiple_of(large * 384 + medium * 320 + i * 256, 64), 256)
            return c

        lax.fori_loop(0, count - large - medium, plain, 0)
        done = flags[3] // 8
        gather(e + 1, 1 - slot, done)
        flags[4] = jnp.maximum(done, groups_of(e + 1))
        return carry

    lax.fori_loop(0, entries, per_expert, 0)
    gather_wait(lax.rem(entries, 2), flags[4])
    for par in range(2):
        y_drain(par)


def combine_kernel(cfg, meta, addr, y, part, acc, ybuf, ysem, osem):
    E, S, CAP, KB, MAXR, T, DEPTH, WIDTH = cfg
    PIECE = 32
    seg_rows = CAP // 8 * KB * PITCH
    piece_rows = PIECE // 8 * KB * PITCH

    def fetch(q, start):
        slot = lax.rem(q, DEPTH)
        s = q // E
        e = q - s * E
        pieces = (meta[e * LANES + s] + PIECE - 1) // PIECE
        base = pl.multiple_of((e * MAXR + meta[e * LANES + S + s]) // 8 * (KB * PITCH), 8)

        def one(i, c):
            src = y.at[pl.ds(pl.multiple_of(base + i * piece_rows, 8), piece_rows)]
            dst = ybuf.at[pl.ds(pl.multiple_of(slot * seg_rows + i * piece_rows, 8), piece_rows)]
            copy = pltpu.make_async_copy(src, dst, ysem.at[slot])
            copy.start() if start else copy.wait()
            return c

        lax.fori_loop(0, pieces, one, 0)

    for q in range(DEPTH - 1):
        fetch(q, True)
    zero = jnp.zeros((8 * KB, LANES), F32)
    for s in range(S):
        a = s % 2
        if s >= 2:
            pltpu.make_async_copy(acc.at[a, pl.ds(0, T * KB)], part.at[s - 2], osem.at[a]).wait()

        def clear(i, c):
            acc[a, pl.ds(pl.multiple_of(i * 8 * KB, 8), 8 * KB), :] = zero
            return c

        lax.fori_loop(0, T // 8, clear, 0)

        def per_expert(e, c):
            q = s * E + e

            @pl.when(q + DEPTH - 1 < S * E)
            def _():
                fetch(q + DEPTH - 1, True)

            fetch(q, False)
            slot_base = lax.rem(q, DEPTH) * seg_rows

            def group(i, cc):
                first = q * WIDTH + i * 16
                rows = [pl.multiple_of(addr[first + k], 8) for k in range(16)]
                at = [slot_base + (i * 2 + k // 8) * (KB * PITCH) + k % 8 for k in range(16)]
                sums = [acc[a, pl.ds(rows[k], KB), :] + ybuf[pl.ds(at[k], KB, stride=PITCH), :] for k in range(16)]
                for k in range(16):
                    acc[a, pl.ds(rows[k], KB), :] = sums[k]
                return cc

            lax.fori_loop(0, (meta[e * LANES + s] + 15) // 16, group, 0)
            return c

        lax.fori_loop(0, E, per_expert, 0)
        pltpu.make_async_copy(acc.at[a, pl.ds(0, T * KB)], part.at[s], osem.at[a]).start()
    for s in range(max(S - 2, 0), S):
        pltpu.make_async_copy(acc.at[s % 2, pl.ds(0, T * KB)], part.at[s], osem.at[s % 2]).wait()


def prep_kernel(KB, *refs):
    resid, moe, attn, router = refs[:4]
    u3, nattn, logits, xs = refs[-4:]
    x = resid[...].astype(F32)
    rows = x.shape[0]
    inv = lax.rsqrt(jnp.mean(x * x, axis=-1, keepdims=True) + EPS)
    x = x * inv
    nattn[...] = (x * attn[...].astype(F32)).astype(BF16)
    u = (x * moe[...].astype(F32)).astype(BF16)
    logits[...] = lax.dot_general(router[...], u, (((1,), (1,)), ((), ())), preferred_element_type=F32)
    wide = u.astype(F32)
    for rb in range(rows // 8):
        for k in range(KB):
            xs[pl.ds(rb * 8 * (KB + 1) + k, 8, stride=KB + 1), :] = wide[rb * 8:rb * 8 + 8, k * LANES:(k + 1) * LANES]
    for r in range(rows):
        u3[r] = xs[r * (KB + 1):r * (KB + 1) + KB, :].astype(BF16)


def run_prep(low, high, rows, resid, moe, attn, router_t, earlier):
    total, D = resid.shape
    KB = D // LANES
    experts = router_t.shape[0]
    first = low // rows
    row_block = pl.BlockSpec((rows, D), lambda i: (first + i, 0))
    scale = pl.BlockSpec((1, D), lambda i: (0, 0))
    args = [resid, moe.reshape(1, D), attn.reshape(1, D), router_t]
    specs = [row_block, scale, scale, pl.BlockSpec((experts, D), lambda i: (0, 0))]
    aliases = {}
    if earlier is not None:
        args += list(earlier)
        specs += [pl.BlockSpec(memory_space=pl.ANY)] * 2
        aliases = {4: 1, 5: 2}
    return pl.pallas_call(
        functools.partial(prep_kernel, KB),
        grid=((high - low) // rows,),
        out_shape=(jax.ShapeDtypeStruct((high - low, KB, LANES), BF16), jax.ShapeDtypeStruct((total, D), BF16), jax.ShapeDtypeStruct((experts, total), F32)),
        in_specs=specs,
        out_specs=(pl.BlockSpec((rows, KB, LANES), lambda i: (i, 0, 0)), row_block, pl.BlockSpec((experts, rows), lambda i: (0, first + i))),
        scratch_shapes=[pltpu.VMEM((rows * (KB + 1), LANES), F32)],
        input_output_aliases=aliases,
        compiler_params=pltpu.CompilerParams(vmem_limit_bytes=66_000_000),
        cost_estimate=pl.CostEstimate(flops=3_000_000_000, bytes_accessed=20_000_000, transcendentals=0),
        name='prep',
    )(*args)


def route_kernel(cfg, ids, logits, table, marks, highs, mids, lows, begins, owners):
    E, T, CAP, NB, SP = cfg
    experts = lax.broadcasted_iota(jnp.int32, (E, T), 0)
    picked = ids[0:1, :] == experts
    for j in range(1, ids.shape[0]):
        picked = jnp.logical_or(picked, ids[j:j + 1, :] == experts)
    masked = jnp.where(picked, logits[...], NEG)
    grown = jnp.where(picked, jnp.exp(masked - jnp.max(masked, axis=0, keepdims=True)), 0.0)
    gates = grown / jnp.sum(grown, axis=0, keepdims=True)
    flags = picked.astype(F32)
    row = lax.broadcasted_iota(jnp.int32, (LANES, LANES), 0)
    col = lax.broadcasted_iota(jnp.int32, (LANES, LANES), 1)
    tri = (row <= col).astype(F32).astype(BF16)
    lane48 = lax.broadcasted_iota(jnp.int32, (E, LANES), 1)
    start = jnp.zeros((E, 1), F32)
    starts = jnp.zeros((E, LANES), F32)
    ends = jnp.zeros((E, LANES), F32)
    for ref in (marks, highs, mids, lows, begins, owners):
        ref[...] = jnp.zeros(ref.shape, F32)
    for b in range(NB):
        cols = slice(b * LANES, (b + 1) * LANES)
        f = flags[:, cols]
        upto = jnp.dot(f.astype(BF16), tri, preferred_element_type=F32)
        g = gates[:, cols]
        high = g.astype(BF16).astype(F32)
        mid = (g - high).astype(BF16).astype(F32)
        low = g - high - mid
        at = slice(b * SP, b * SP + E)
        marks[at, :] = f * upto
        highs[at, :] = high
        mids[at, :] = mid
        lows[at, :] = low
        begins[at, :] = jnp.broadcast_to(start, (E, LANES))
        owners[at, :] = jnp.full((E, LANES), float(b), F32)
        end = start + upto[:, LANES - 1:LANES]
        here = lane48 % 16 == b
        starts = jnp.where(here, start, starts)
        ends = jnp.where(here, end, ends)
        start = end
    rank = lax.broadcasted_iota(jnp.int32, (CAP, LANES), 0).astype(F32)
    lane = lax.broadcasted_iota(jnp.int32, (CAP, LANES), 1)
    lane_f = lane.astype(F32)
    total = start
    out = jnp.zeros((CAP, LANES), F32)
    for e in range(E):
        def rows_at(ref):
            return ref[pl.ds(e, 16, stride=SP), :]
        begin = rows_at(begins)
        over = jnp.where(begin >= 512.0, 512.0, jnp.where(begin >= 256.0, 256.0, 0.0))
        zero = jnp.zeros((16, 4 * LANES), F32)
        first = jnp.concatenate([rows_at(marks), rows_at(highs), rows_at(mids), rows_at(lows), rows_at(owners)], axis=1)
        second = jnp.concatenate([begin - over, zero], axis=1)
        third = jnp.concatenate([over, zero], axis=1)
        grid = jnp.concatenate([first, second, third, jnp.zeros((LANES - 48, 5 * LANES), F32)], axis=0).astype(BF16)
        mine = jnp.logical_and(rank >= starts[e:e + 1], rank < ends[e:e + 1])
        hot = jnp.where(jnp.logical_and(mine, lane < 48), 1.0, 0.0).astype(BF16)
        got = jnp.dot(hot, grid, preferred_element_type=F32)
        same = got[:, :LANES] == rank + 1.0
        gate = jnp.where(same, got[:, LANES:2 * LANES] + got[:, 2 * LANES:3 * LANES] + got[:, 3 * LANES:4 * LANES], 0.0)
        token = jnp.where(same, lane_f + float(LANES) * got[:, 4 * LANES:], 0.0)
        gate = jnp.sum(gate, axis=1, keepdims=True)
        token = jnp.sum(token, axis=1, keepdims=True)
        token = jnp.where(rank[:, :1] < total[e:e + 1], token, float(T))
        out = jnp.where(lane == e, token, out)
        out = jnp.where(lane == LANES // 2 + e, gate, out)
    pad = jnp.zeros((table.shape[1] - CAP, LANES), F32)
    table[...] = jnp.concatenate([out, pad], axis=0).T


def run_route(ids, logits, cap):
    E, T = logits.shape
    NB = T // LANES
    SP = E + 1 if E % 8 == 0 else E
    wide = -(-cap // LANES) * LANES
    rows = 16 * SP
    return pl.pallas_call(
        functools.partial(route_kernel, (E, T, cap, NB, SP)),
        out_shape=jax.ShapeDtypeStruct((LANES, wide), F32),
        in_specs=[pl.BlockSpec(memory_space=pltpu.VMEM)] * 2,
        out_specs=pl.BlockSpec(memory_space=pltpu.VMEM),
        scratch_shapes=[pltpu.VMEM((rows, LANES), F32)] * 6,
        compiler_params=pltpu.CompilerParams(vmem_limit_bytes=66_000_000),
        cost_estimate=pl.CostEstimate(flops=10_000_000_000, bytes_accessed=2_000_000, transcendentals=0),
        name='route',
    )(ids, logits)


def lists_kernel(cfg, table, lst, gcol, meta, addr):
    S, E, CAP, T, KB, MAXR, WIDE = cfg
    width = table.shape[3]
    lane = lax.broadcasted_iota(jnp.int32, (E, width), 1)
    start = jnp.zeros((E, 1), jnp.int32)
    rows_all = jnp.zeros((E, WIDE), F32)
    gates_all = jnp.zeros((E, WIDE), F32)
    meta_lane = lax.broadcasted_iota(jnp.int32, (E, LANES), 1)
    facts = jnp.zeros((E, LANES), jnp.int32)
    for s in range(S):
        tok = table[0, s]
        gate = table[1, s]
        valid = jnp.logical_and(tok < float(T), lane < CAP)
        cnt = jnp.sum(jnp.where(valid, 1.0, 0.0), axis=1, keepdims=True).astype(jnp.int32)
        addr[s] = jnp.where(valid, tok, float(T)).astype(jnp.int32) * KB
        rows = jnp.where(valid, tok + float(s * T), 0.0)
        gate = jnp.where(valid, gate, 0.0)
        blank = jnp.zeros((E, WIDE - width), F32)
        rows = jnp.concatenate([rows, blank], axis=1)
        gate = jnp.concatenate([gate, blank], axis=1)
        bit = 8
        while bit < MAXR:
            take = (start // bit) % 2 == 1
            rows = jnp.where(take, pltpu.roll(rows, bit, 1), rows)
            gate = jnp.where(take, pltpu.roll(gate, bit, 1), gate)
            bit *= 2
        rows_all = rows_all + rows
        gates_all = gates_all + gate
        facts = jnp.where(meta_lane == s, cnt, facts)
        facts = jnp.where(meta_lane == S + s, start, facts)
        start = start + (cnt + 7) // 8 * 8
    facts = jnp.where(meta_lane == 2 * S, start, facts)
    pad = meta.shape[0] - E
    meta[...] = jnp.concatenate([facts, jnp.zeros((pad, LANES), jnp.int32)], axis=0)
    lst[...] = jnp.concatenate([rows_all.astype(jnp.int32), jnp.zeros((pad, WIDE), jnp.int32)], axis=0)
    square = jnp.concatenate([gates_all, jnp.zeros((LANES - E, WIDE), F32)], axis=0)
    for c in range(WIDE // LANES):
        turned = square[:, c * LANES:(c + 1) * LANES].T
        for e in range(E):
            gcol[e, c * LANES:(c + 1) * LANES, :] = jnp.broadcast_to(turned[:, e:e + 1], (LANES, LANES))


def run_lists(table, cap, T, KB):
    _, S, E, width = table.shape
    MAXR = S * cap
    WIDE = MAXR + LANES
    rows = E + 8
    vmem = pl.BlockSpec(memory_space=pltpu.VMEM)
    return pl.pallas_call(
        functools.partial(lists_kernel, (S, E, cap, T, KB, MAXR, WIDE)),
        out_shape=(jax.ShapeDtypeStruct((rows, WIDE), jnp.int32), jax.ShapeDtypeStruct((E, WIDE, LANES), F32), jax.ShapeDtypeStruct((rows, LANES), jnp.int32), jax.ShapeDtypeStruct((S, E, width), jnp.int32)),
        in_specs=[vmem],
        out_specs=(vmem,) * 4,
        compiler_params=pltpu.CompilerParams(vmem_limit_bytes=66_000_000),
        cost_estimate=pl.CostEstimate(flops=10_000_000_000, bytes_accessed=22_000_000, transcendentals=0),
        name='lists',
    )(table)


def attention_kernel(seq, q_ref, k_ref, v_ref, cos_ref, sin_ref, cos_t, sin_t, o_ref):
    step = 128
    half = LANES // 2
    key = lax.broadcasted_iota(jnp.int32, (step, step), 0)
    query = lax.broadcasted_iota(jnp.int32, (step, step), 1)
    keep = query >= key
    factor = LANES ** -0.5 * 1.4426950408889634
    for hh in range(k_ref.shape[1] // LANES):
        at = hh * LANES
        first, second = q_ref[at:at + half, :], q_ref[at + half:at + LANES, :]
        ct, st = cos_t[...], sin_t[...]
        q = jnp.concatenate([first * ct - second * st, second * ct + first * st], axis=0).astype(BF16)
        kf = k_ref[:, at:at + LANES]
        k = (kf * cos_ref[...] + pltpu.roll(kf, half, 1) * sin_ref[...]).astype(BF16)
        v = v_ref[at:at + LANES, :]
        for j in range(seq // step):
            n = (j + 1) * step
            s = jnp.dot(k[:n], q[:, j * step:n], preferred_element_type=F32)
            diag = jnp.where(keep, s[j * step:], NEG)
            s = jnp.concatenate([s[:j * step], diag], axis=0) if j else diag
            p = jnp.exp2((s - jnp.max(s, axis=0, keepdims=True)) * factor)
            p = (p * (1.0 / jnp.sum(p, axis=0, keepdims=True))).astype(BF16)
            o_ref[at:at + LANES, j * step:n] = jnp.dot(v[:, :n], p, preferred_element_type=F32).astype(BF16)


def run_attention(q_t, k, v_t, seq):
    T, D = k.shape
    half = LANES // 2
    freqs = ROPE_BASE ** (-jnp.arange(half, dtype=F32) * 2.0 / LANES)
    angles = jnp.arange(seq, dtype=F32)[:, None] * freqs[None, :]
    cos_half, sin_half = jnp.cos(angles), jnp.sin(angles)
    cosine = jnp.concatenate([cos_half, cos_half], axis=1)
    sine = jnp.concatenate([-sin_half, sin_half], axis=1)
    wide = min(D, 512)
    block = pl.BlockSpec((seq, wide), lambda i, j: (i, j))
    block_t = pl.BlockSpec((wide, seq), lambda i, j: (j, i))
    table = pl.BlockSpec((seq, LANES), lambda i, j: (0, 0))
    table_t = pl.BlockSpec((half, seq), lambda i, j: (0, 0))
    return pl.pallas_call(
        functools.partial(attention_kernel, seq),
        grid=(T // seq, D // wide),
        out_shape=jax.ShapeDtypeStruct((D, T), BF16),
        in_specs=[block_t, block, block_t, table, table, table_t, table_t],
        out_specs=block_t,
        compiler_params=pltpu.CompilerParams(vmem_limit_bytes=66_000_000),
        cost_estimate=pl.CostEstimate(flops=50_000_000_000, bytes_accessed=76_000_000, transcendentals=0),
        name='attention',
    )(q_t, k, v_t, cosine, sine, cos_half.T, sin_half.T)


def final_kernel(KB, b, m, *rest):
    o = rest[-1]
    rows = b.shape[0]
    for k in range(KB):
        cols = slice(k * LANES, (k + 1) * LANES)
        o[:, cols] = (b[:, cols] + m[pl.ds(k, rows, stride=KB), :]).astype(BF16)


def run_final(low, high, rows, b, m, earlier):
    total, D = b.shape
    KB = D // LANES
    first = low // rows
    args = [b, m]
    specs = [pl.BlockSpec((rows, D), lambda i: (first + i, 0)), pl.BlockSpec((rows * KB, LANES), lambda i: (i, 0))]
    aliases = {}
    if earlier is not None:
        args.append(earlier)
        specs.append(pl.BlockSpec(memory_space=pl.ANY))
        aliases = {2: 0}
    return pl.pallas_call(
        functools.partial(final_kernel, KB),
        grid=((high - low) // rows,),
        out_shape=jax.ShapeDtypeStruct((total, D), BF16),
        in_specs=specs,
        out_specs=pl.BlockSpec((rows, D), lambda i: (first + i, 0)),
        input_output_aliases=aliases,
        compiler_params=pltpu.CompilerParams(vmem_limit_bytes=66_000_000),
        cost_estimate=pl.CostEstimate(flops=1_000_000_000, bytes_accessed=32_000_000, transcendentals=0),
        name='final',
    )(*args)


def run_experts(meta, lst, gcol, u, own, other):
    E, MAXR = gcol.shape[0], gcol.shape[1] - LANES
    D, FE = own[0].shape[1], own[0].shape[2]
    KB = D // LANES
    sizes = (256, 320, 384)
    limit = min(MAXR, 1152)
    cfg = (E, KB, FE, MAXR, lst.shape[1], limit, sizes)
    entries = E * -(-MAXR // limit) + 2
    any_spec = pl.BlockSpec(memory_space=pl.ANY)
    smem = pl.BlockSpec(memory_space=pltpu.SMEM)
    return pl.pallas_call(
        functools.partial(expert_kernel, cfg),
        out_shape=jax.ShapeDtypeStruct(((E * MAXR + 32) // 8 * KB * PITCH, LANES), F32),
        in_specs=[smem, smem] + [any_spec] * 8,
        out_specs=any_spec,
        scratch_shapes=[
            pltpu.VMEM((2, D, FE), BF16), pltpu.VMEM((2, D, FE), BF16), pltpu.VMEM((2, FE, D), BF16), pltpu.VMEM((2 * limit, LANES), F32),
            pltpu.VMEM((2 * limit, KB, LANES), BF16), pltpu.VMEM((32 * (KB + 1), LANES), F32), pltpu.VMEM((max(sizes) // 16, KB, 16, LANES), BF16),
            pltpu.VMEM((max(sizes), FE), BF16), pltpu.VMEM((2 * max(sizes) // 8 * KB * PITCH, LANES), F32), pltpu.SMEM((5,), jnp.int32), pltpu.SMEM((3 * entries,), jnp.int32),
            pltpu.SemaphoreType.DMA((2,)), pltpu.SemaphoreType.DMA((2,)), pltpu.SemaphoreType.DMA((2,)),
        ],
        compiler_params=pltpu.CompilerParams(vmem_limit_bytes=66_000_000),
        cost_estimate=pl.CostEstimate(flops=E * MAXR * D * FE * 3, bytes_accessed=400_000_000, transcendentals=0),
        name='experts',
    )(meta.reshape(-1), lst.reshape(-1), gcol, u, *own, *other)


def run_combine(meta, addr, y, T, KB, cap):
    chips, E, width = addr.shape
    MAXR = chips * cap
    DEPTH = 4
    cfg = (E, chips, cap, KB, MAXR, T, DEPTH, width)
    smem = pl.BlockSpec(memory_space=pltpu.SMEM)
    any_spec = pl.BlockSpec(memory_space=pl.ANY)
    return pl.pallas_call(
        functools.partial(combine_kernel, cfg),
        out_shape=jax.ShapeDtypeStruct((chips, T * KB, LANES), F32),
        in_specs=[smem, smem, any_spec],
        out_specs=any_spec,
        scratch_shapes=[
            pltpu.VMEM((2, (T + 8) * KB, LANES), F32), pltpu.VMEM((DEPTH * (cap // 8) * KB * PITCH, LANES), F32),
            pltpu.SemaphoreType.DMA((DEPTH,)), pltpu.SemaphoreType.DMA((2,)),
        ],
        compiler_params=pltpu.CompilerParams(vmem_limit_bytes=66_000_000),
        cost_estimate=pl.CostEstimate(flops=40_000_000_000, bytes_accessed=150_000_000, transcendentals=0),
        name='combine',
    )(meta.reshape(-1), addr.reshape(-1), y)


def solution(mesh):
    group_size = mesh.shape['ep']
    tok_spec = P(None, ('dp', 'ep'), None, None)
    rep_one = P(None)
    rep_two = P(None, None)
    rep_three = P(None, None, None)
    expert_spec = P('ep', None, None)
    chips = group_size // 2
    same_core = [[2 * c for c in range(chips)], [2 * c + 1 for c in range(chips)]]
    partner = [(i, i ^ 1) for i in range(group_size)]

    def local_program(resid_in, expert_idx, expert_slot, w_query, w_key, w_value, w_out, w_gate, w_up, w_down, w_router, norm_attn, norm_ffn, norm_moe, expert_gate, expert_up, expert_down):
        micros, seqs, seq_len, width = resid_in.shape
        T = seqs * seq_len
        KB = width // LANES
        choices = expert_idx.shape[-1]
        local_experts = expert_gate.shape[0]
        experts = local_experts * group_size
        E = 2 * local_experts
        cap = CAP_FACTOR * T * choices // experts
        me = lax.axis_index('ep')
        own = (expert_gate, expert_up, expert_down)
        other = tuple(lax.ppermute(w, 'ep', partner) for w in own)

        total = micros * T
        resid = resid_in.reshape(total, width)
        rows = min(256, T // 2)
        split = int(total * FIRST_SHARE) // rows * rows
        chunks = []
        for low, high in ((0, split), (split, total)):
            held = sum(min(cap, max(0, min(high, (m + 1) * T) - max(low, m * T))) for m in range(micros))
            chunks.append((low, high, held))
        router_t = w_router.T
        tokens_all, nattn, logits = [], None, None
        for low, high, _ in chunks:
            u3, nattn, logits = run_prep(low, high, rows, resid, norm_moe, norm_attn, router_t, (nattn, logits) if low else None)
            tokens_all.append(lax.all_gather(u3, 'ep', axis_index_groups=same_core))
        ids = expert_idx.reshape(total, choices).T
        tables = [run_route(ids[:, low:high], logits[:, low:high], held) for low, high, held in chunks]
        widths = [t.shape[1] for t in tables]
        table = jnp.concatenate(tables, axis=1).reshape(2, LANES // 2, -1)[:, :experts].reshape(2, chips, E, -1)
        table = lax.all_to_all(table, 'ep', 1, 1, tiled=True, axis_index_groups=same_core)
        core = lax.rem(me, 2)
        table = jnp.concatenate([lax.dynamic_slice_in_dim(table, core * local_experts, local_experts, 2), lax.dynamic_slice_in_dim(table, (1 - core) * local_experts, local_experts, 2)], 2)
        plans, at = [], 0
        for (low, high, held), wide in zip(chunks, widths):
            plans.append(run_lists(table[:, :, :, at:at + wide], held, high - low, KB))
            at += wide

        across = (((0,), (1,)), ((), ()))
        q_t = lax.dot_general(w_query.reshape(width, -1), nattn, across, preferred_element_type=F32)
        k = jnp.dot(nattn, w_key.reshape(width, -1), preferred_element_type=F32)
        v_t = lax.dot_general(w_value.reshape(width, -1), nattn, across, preferred_element_type=F32).astype(BF16)

        summed = []
        for (low, high, held), tokens, (lst, gcol, meta, addr) in zip(chunks, tokens_all, plans):
            count = high - low
            if low == 0:
                meta, q_t, k, v_t = lax.optimization_barrier((meta, q_t, k, v_t))
            y = run_experts(meta, lst, gcol, tokens.reshape(chips * count, KB, LANES), own, other)
            part = run_combine(meta, addr, y, count, KB, held)
            if high == total:
                part, q_t, k, v_t = lax.optimization_barrier((part, q_t, k, v_t))
            summed.append(lax.psum_scatter(part, 'ep', scatter_dimension=0, axis_index_groups=same_core))
        o_t = run_attention(q_t, k, v_t, seq_len)
        attn_out = lax.dot_general(o_t, w_out.reshape(-1, width), (((0,), (0,)), ((), ())), preferred_element_type=F32)
        after = (resid.astype(F32) + attn_out).astype(BF16)
        dense = ffn_branch(after, norm_ffn, w_gate, w_up, w_down)
        out = None
        for (low, high, _), moe in zip(chunks, summed):
            out = run_final(low, high, rows, dense, moe.reshape((high - low) * KB, LANES), out)
        return out.reshape(micros, seqs, seq_len, width)

    return jax.shard_map(local_program, mesh=mesh, in_specs=(tok_spec, tok_spec, tok_spec, rep_three, rep_three, rep_three, rep_three, rep_two, rep_two, rep_two, rep_two, rep_one, rep_one, rep_one, expert_spec, expert_spec, expert_spec), out_specs=tok_spec, check_vma=False)
```

```python
import functools

import jax
import jax.numpy as jnp
from jax import lax
from jax.experimental import pallas as pl
from jax.experimental.pallas import tpu as pltpu
from jax.sharding import PartitionSpec as P

EPS = 1e-6
ROPE_BASE = 10000.0
CAP_FACTOR = 2
NEG = -1e30
LANES = 128
PITCH = 9
STEP = 16
VMEM_ALL = 66_000_000
WIDE_TILE = 256
SLOTS = 3
FIRST_SHARE = 0.42
F32 = jnp.float32
BF16 = jnp.bfloat16


def rms_norm(values, scale):
    widened = values.astype(F32)
    mean_sq = jnp.mean(widened * widened, axis=-1, keepdims=True)
    return (widened * lax.rsqrt(mean_sq + EPS) * scale.astype(F32)).astype(BF16)


def ffn_branch(after_attn, norm_ffn, w_gate, w_up, w_down):
    normed_ffn = rms_norm(after_attn, norm_ffn)
    gate_act = jnp.dot(normed_ffn, w_gate, preferred_element_type=F32)
    up_act = jnp.dot(normed_ffn, w_up, preferred_element_type=F32)
    hidden = (gate_act * jax.nn.sigmoid(gate_act) * up_act).astype(BF16)
    return after_attn.astype(F32) + jnp.dot(hidden, w_down, preferred_element_type=F32)


def expert_kernel(cfg, meta, lst, gates, u, wg0, wu0, wd0, wg1, wu1, wd1, y, wg, wu, wd, x3, xs, x2, h, yb, flags, pending, plan, wsem, xsem, ysem):
    E, KB, FE, MAXR, WIDE, LIMIT, SIZES = cfg
    ENTRIES = plan.shape[0] // 3
    YROWS = max(SIZES) // 8 * KB * PITCH
    half = E // 2
    D = KB * LANES

    def expert_of(v):
        return plan[v]

    def first_of(v):
        return plan[ENTRIES + v]

    def groups_of(v):
        return plan[2 * ENTRIES + v]

    def weights(v, slot, start):
        if not start:
            pltpu.make_async_copy(wg0.at[0], wg.at[slot], wsem.at[slot]).wait()
            pltpu.make_async_copy(wu0.at[0], wu.at[slot], wsem.at[slot]).wait()
            pltpu.make_async_copy(wd0.at[0], wd.at[slot], wsem.at[slot]).wait()
            return

        e = expert_of(v)

        @pl.when(e < half)
        def _():
            pltpu.make_async_copy(wg0.at[e], wg.at[slot], wsem.at[slot]).start()
            pltpu.make_async_copy(wu0.at[e], wu.at[slot], wsem.at[slot]).start()
            pltpu.make_async_copy(wd0.at[e], wd.at[slot], wsem.at[slot]).start()

        @pl.when(e >= half)
        def _():
            pltpu.make_async_copy(wg1.at[e - half], wg.at[slot], wsem.at[slot]).start()
            pltpu.make_async_copy(wu1.at[e - half], wu.at[slot], wsem.at[slot]).start()
            pltpu.make_async_copy(wd1.at[e - half], wd.at[slot], wsem.at[slot]).start()

    def copy_row(index, slot, r):
        pltpu.make_async_copy(u.at[lst[index]], x3.at[slot * LIMIT + r], xsem.at[slot]).start()

    def gather(v, begin):
        slot = lax.rem(v, SLOTS)
        base = expert_of(v) * WIDE + first_of(v)
        steps = (groups_of(v) + 1) // 2

        def issue(i, carry):
            for k in range(STEP):
                copy_row(base + i * STEP + k, slot, i * STEP + k)
            return carry

        lax.fori_loop(begin, steps, issue, 0)
        pending[slot] = jnp.maximum(begin, steps)

    def gather_wait(v):
        slot = lax.rem(v, SLOTS)
        steps = pending[slot]
        for rows in (4 * STEP, STEP):
            def one(i, carry, rows=rows):
                pltpu.make_async_copy(u.at[pl.ds(0, rows)], x3.at[pl.ds(0, rows)], xsem.at[slot]).wait()
                return carry

            lax.fori_loop(0, lax.rem(steps, 4) if rows == STEP else steps // 4, one, 0)

    def y_copy(rows, par, dst):
        n = rows // 8 * KB * PITCH
        return pltpu.make_async_copy(yb.at[pl.ds(pl.multiple_of(par * YROWS, 8), n)], y.at[pl.ds(dst, n)], ysem.at[par])

    def y_drain(par):
        for which, rows in enumerate(SIZES):
            @pl.when(flags[par] == which + 1)
            def _(rows=rows):
                y_copy(rows, par, 0).wait()

    def block(v, slot, r0, M):
        src = lax.rem(v, SLOTS) * LIMIT + r0
        par = flags[2]
        y_drain(par)
        flags[par] = SIZES.index(M) + 1
        flags[2] = 1 - par
        ybase = par * YROWS
        issued = flags[3]
        flags[3] = issued + M
        later = lax.rem(v + 2, SLOTS)
        base = expert_of(v + 2) * WIDE + first_of(v + 2) + issued
        parts = -(-FE // WIDE_TILE) + D // WIDE_TILE

        def ahead(part):
            for r in range(M * part // parts, M * (part + 1) // parts):
                copy_row(base + r, later, issued + r)

        weight = jnp.sum(jnp.where(lax.broadcasted_iota(jnp.int32, (M, LANES), 1) == expert_of(v), gates[pl.ds(pl.multiple_of(first_of(v) + r0, 8), M), :], 0.0), axis=1, keepdims=True)

        def relayout(g, carry):
            for i in range(32):
                xs[i * (KB + 1):i * (KB + 1) + KB, :] = x3[src + g * 32 + i].astype(F32)
            for half in range(2):
                for k in range(KB):
                    x2[g * 2 + half, k] = xs[pl.ds(half * 16 * (KB + 1) + k, 16, stride=KB + 1), :].astype(BF16)
            return carry

        lax.fori_loop(0, M // 32, relayout, 0)
        x = jnp.concatenate([x2[0:M // 16, k].reshape(M, LANES) for k in range(KB)], axis=1)
        full = FE // WIDE_TILE
        for j in range(full):
            cols = slice(j * WIDE_TILE, j * WIDE_TILE + WIDE_TILE)
            ga = jnp.dot(x, wg[slot, :, cols], preferred_element_type=F32)
            ua = jnp.dot(x, wu[slot, :, cols], preferred_element_type=F32)
            h[0:M, cols] = (ga * jax.nn.sigmoid(ga) * ua).astype(BF16)
            ahead(j)
        if FE % WIDE_TILE:
            ahead(full)
            cols = slice(full * WIDE_TILE, FE)
            width = FE - full * WIDE_TILE
            both = jnp.dot(x, jnp.concatenate([wg[slot, :, cols], wu[slot, :, cols]], axis=1), preferred_element_type=F32)
            ga, ua = both[:, :width], both[:, width:]
            h[0:M, cols] = (ga * jax.nn.sigmoid(ga) * ua).astype(BF16)
        hid = h[0:M, :]
        for j in range(D // WIDE_TILE):
            out = jnp.dot(hid, wd[slot, :, j * WIDE_TILE:j * WIDE_TILE + WIDE_TILE], preferred_element_type=F32)
            out = weight * out.astype(BF16).astype(F32)
            ahead(parts - D // WIDE_TILE + j)
            for rb in range(M // 8):
                for k in range(2):
                    at = (rb * KB + 2 * j + k) * PITCH
                    yb[pl.ds(ybase + at, 8), :] = out[rb * 8:rb * 8 + 8, k * LANES:(k + 1) * LANES]
        dst = pl.multiple_of((expert_of(v) * MAXR + first_of(v) + r0) // 8 * (KB * PITCH), 8)
        y_copy(M, par, dst).start()

    flags[0] = 0
    flags[1] = 0
    flags[2] = 0
    def blank(i, carry):
        plan[i] = 0
        return carry

    lax.fori_loop(0, 3 * ENTRIES, blank, 0)

    def add(e, at):
        groups = meta[e * LANES + 8] // 8
        for part in range(-(-MAXR // LIMIT)):
            take = jnp.clip(groups - part * (LIMIT // 8), 0, LIMIT // 8)

            @pl.when(take > 0)
            def _(part=part, take=take, at=at):
                plan[at] = e
                plan[ENTRIES + at] = part * LIMIT
                plan[2 * ENTRIES + at] = take

            at = at + (take > 0).astype(jnp.int32)
        return at

    entries = jnp.maximum(lax.fori_loop(0, E, add, jnp.int32(0)), 1)
    gather(0, 0)
    weights(0, 0, True)
    gather(1, 0)

    def per_expert(e, carry):
        slot = lax.rem(e, 2)
        weights(e, slot, False)
        gather_wait(e)
        flags[3] = 0

        @pl.when(e + 1 < entries)
        def _():
            weights(e + 1, 1 - slot, True)

        units = (groups_of(e) + 7) // 8
        count = jnp.where(units == 7, 2, units // 4)
        rest = jnp.where(units == 7, 0, lax.rem(units, 4))
        rest = jnp.where(units < 4, 0, rest)
        count = jnp.where(jnp.logical_and(units > 0, units < 4), 1, count)
        large = (rest >= 2).astype(jnp.int32)
        medium = lax.rem(rest, 2)

        @pl.when(large == 1)
        def _():
            block(e, slot, 0, 384)

        @pl.when(medium == 1)
        def _():
            block(e, slot, pl.multiple_of(large * 384, 64), 320)

        def plain(i, c):
            block(e, slot, pl.multiple_of(large * 384 + medium * 320 + i * WIDE_TILE, 64), WIDE_TILE)
            return c

        lax.fori_loop(0, count - large - medium, plain, 0)
        gather(e + 2, flags[3] // STEP)
        return carry

    lax.fori_loop(0, entries, per_expert, 0)
    for par in range(2):
        gather_wait(entries + par)
        y_drain(par)


def combine_kernel(cfg, meta, addr, y, part, acc, ybuf, ysem, osem):
    E, S, CAP, KB, MAXR, T, DEPTH, WIDTH = cfg
    PIECE = 32
    seg_rows = CAP // 8 * KB * PITCH
    piece_rows = PIECE // 8 * KB * PITCH

    def fetch(q, start):
        slot = lax.rem(q, DEPTH)
        s = q // E
        e = q - s * E
        pieces = (meta[e * LANES + s] + PIECE - 1) // PIECE
        base = pl.multiple_of((e * MAXR + meta[e * LANES + S + s]) // 8 * (KB * PITCH), 8)

        def one(i, c):
            src = y.at[pl.ds(pl.multiple_of(base + i * piece_rows, 8), piece_rows)]
            dst = ybuf.at[pl.ds(pl.multiple_of(slot * seg_rows + i * piece_rows, 8), piece_rows)]
            copy = pltpu.make_async_copy(src, dst, ysem.at[slot])
            copy.start() if start else copy.wait()
            return c

        lax.fori_loop(0, pieces, one, 0)

    for q in range(DEPTH - 1):
        fetch(q, True)
    zero = jnp.zeros((8 * KB, LANES), F32)
    for s in range(S):
        a = s % 2
        if s >= 2:
            pltpu.make_async_copy(acc.at[a, pl.ds(0, T * KB)], part.at[s - 2], osem.at[a]).wait()

        def clear(i, c):
            acc[a, pl.ds(pl.multiple_of(i * 8 * KB, 8), 8 * KB), :] = zero
            return c

        lax.fori_loop(0, T // 8, clear, 0)

        def per_expert(e, c):
            q = s * E + e

            @pl.when(q + DEPTH - 1 < S * E)
            def _():
                fetch(q + DEPTH - 1, True)

            fetch(q, False)
            slot_base = lax.rem(q, DEPTH) * seg_rows

            def group(i, cc):
                first = q * WIDTH + i * 16
                rows = [pl.multiple_of(addr[first + k], 8) for k in range(16)]
                at = [slot_base + (i * 2 + k // 8) * (KB * PITCH) + k % 8 for k in range(16)]
                sums = [acc[a, pl.ds(rows[k], KB), :] + ybuf[pl.ds(at[k], KB, stride=PITCH), :] for k in range(16)]
                for k in range(16):
                    acc[a, pl.ds(rows[k], KB), :] = sums[k]
                return cc

            lax.fori_loop(0, (meta[e * LANES + s] + 15) // 16, group, 0)
            return c

        lax.fori_loop(0, E, per_expert, 0)
        pltpu.make_async_copy(acc.at[a, pl.ds(0, T * KB)], part.at[s], osem.at[a]).start()
    for s in range(max(S - 2, 0), S):
        pltpu.make_async_copy(acc.at[s % 2, pl.ds(0, T * KB)], part.at[s], osem.at[s % 2]).wait()


def prep_kernel(KB, *refs):
    resid, moe, attn, router = refs[:4]
    u3, nattn, logits, xs = refs[-4:]
    x = resid[...].astype(F32)
    rows = x.shape[0]
    inv = lax.rsqrt(jnp.mean(x * x, axis=-1, keepdims=True) + EPS)
    x = x * inv
    nattn[...] = (x * attn[...].astype(F32)).astype(BF16)
    u = (x * moe[...].astype(F32)).astype(BF16)
    logits[...] = lax.dot_general(router[...], u, (((1,), (1,)), ((), ())), preferred_element_type=F32)
    wide = u.astype(F32)
    for rb in range(rows // 8):
        for k in range(KB):
            xs[pl.ds(rb * 8 * (KB + 1) + k, 8, stride=KB + 1), :] = wide[rb * 8:rb * 8 + 8, k * LANES:(k + 1) * LANES]
    for r in range(rows):
        u3[r] = xs[r * (KB + 1):r * (KB + 1) + KB, :].astype(BF16)


def run_prep(low, high, rows, resid, moe, attn, router_t, earlier):
    total, D = resid.shape
    KB = D // LANES
    experts = router_t.shape[0]
    first = low // rows
    row_block = pl.BlockSpec((rows, D), lambda i: (first + i, 0))
    scale = pl.BlockSpec((1, D), lambda i: (0, 0))
    args = [resid, moe.reshape(1, D), attn.reshape(1, D), router_t]
    specs = [row_block, scale, scale, pl.BlockSpec((experts, D), lambda i: (0, 0))]
    aliases = {}
    if earlier is not None:
        args += list(earlier)
        specs += [pl.BlockSpec(memory_space=pl.ANY)] * 2
        aliases = {4: 1, 5: 2}
    return pl.pallas_call(
        functools.partial(prep_kernel, KB),
        grid=((high - low) // rows,),
        out_shape=(jax.ShapeDtypeStruct((high - low, KB, LANES), BF16), jax.ShapeDtypeStruct((total, D), BF16), jax.ShapeDtypeStruct((experts, total), F32)),
        in_specs=specs,
        out_specs=(pl.BlockSpec((rows, KB, LANES), lambda i: (i, 0, 0)), row_block, pl.BlockSpec((experts, rows), lambda i: (0, first + i))),
        scratch_shapes=[pltpu.VMEM((rows * (KB + 1), LANES), F32)],
        input_output_aliases=aliases,
        compiler_params=pltpu.CompilerParams(vmem_limit_bytes=VMEM_ALL),
        cost_estimate=pl.CostEstimate(flops=3_000_000_000, bytes_accessed=20_000_000, transcendentals=0),
        name='prep',
    )(*args)


def route_kernel(cfg, ids, logits, table, marks, highs, mids, lows, begins, owners):
    E, T, CAP, NB, SP = cfg
    experts = lax.broadcasted_iota(jnp.int32, (E, T), 0)
    picked = ids[0:1, :] == experts
    for j in range(1, ids.shape[0]):
        picked = jnp.logical_or(picked, ids[j:j + 1, :] == experts)
    masked = jnp.where(picked, logits[...], NEG)
    grown = jnp.where(picked, jnp.exp(masked - jnp.max(masked, axis=0, keepdims=True)), 0.0)
    gates = grown / jnp.sum(grown, axis=0, keepdims=True)
    flags = picked.astype(F32)
    row = lax.broadcasted_iota(jnp.int32, (LANES, LANES), 0)
    col = lax.broadcasted_iota(jnp.int32, (LANES, LANES), 1)
    tri = (row <= col).astype(F32).astype(BF16)
    lane48 = lax.broadcasted_iota(jnp.int32, (E, LANES), 1)
    start = jnp.zeros((E, 1), F32)
    starts = jnp.zeros((E, LANES), F32)
    ends = jnp.zeros((E, LANES), F32)
    for ref in (marks, highs, mids, lows, begins, owners):
        ref[...] = jnp.zeros(ref.shape, F32)
    for b in range(NB):
        cols = slice(b * LANES, (b + 1) * LANES)
        f = flags[:, cols]
        upto = jnp.dot(f.astype(BF16), tri, preferred_element_type=F32)
        g = gates[:, cols]
        high = g.astype(BF16).astype(F32)
        mid = (g - high).astype(BF16).astype(F32)
        low = g - high - mid
        at = slice(b * SP, b * SP + E)
        marks[at, :] = f * upto
        highs[at, :] = high
        mids[at, :] = mid
        lows[at, :] = low
        begins[at, :] = jnp.broadcast_to(start, (E, LANES))
        owners[at, :] = jnp.full((E, LANES), float(b), F32)
        end = start + upto[:, LANES - 1:LANES]
        here = lane48 % 16 == b
        starts = jnp.where(here, start, starts)
        ends = jnp.where(here, end, ends)
        start = end
    rank = lax.broadcasted_iota(jnp.int32, (CAP, LANES), 0).astype(F32)
    lane = lax.broadcasted_iota(jnp.int32, (CAP, LANES), 1)
    lane_f = lane.astype(F32)
    total = start
    out = jnp.zeros((CAP, LANES), F32)
    for e in range(E):
        def rows_at(ref):
            return ref[pl.ds(e, 16, stride=SP), :]
        begin = rows_at(begins)
        over = jnp.where(begin >= 512.0, 512.0, jnp.where(begin >= 256.0, 256.0, 0.0))
        zero = jnp.zeros((16, 4 * LANES), F32)
        first = jnp.concatenate([rows_at(marks), rows_at(highs), rows_at(mids), rows_at(lows), rows_at(owners)], axis=1)
        second = jnp.concatenate([begin - over, zero], axis=1)
        third = jnp.concatenate([over, zero], axis=1)
        grid = jnp.concatenate([first, second, third, jnp.zeros((LANES - 48, 5 * LANES), F32)], axis=0).astype(BF16)
        mine = jnp.logical_and(rank >= starts[e:e + 1], rank < ends[e:e + 1])
        hot = jnp.where(jnp.logical_and(mine, lane < 48), 1.0, 0.0).astype(BF16)
        got = jnp.dot(hot, grid, preferred_element_type=F32)
        same = got[:, :LANES] == rank + 1.0
        gate = jnp.where(same, got[:, LANES:2 * LANES] + got[:, 2 * LANES:3 * LANES] + got[:, 3 * LANES:4 * LANES], 0.0)
        token = jnp.where(same, lane_f + float(LANES) * got[:, 4 * LANES:], 0.0)
        gate = jnp.sum(gate, axis=1, keepdims=True)
        token = jnp.sum(token, axis=1, keepdims=True)
        token = jnp.where(rank[:, :1] < total[e:e + 1], token, float(T))
        out = jnp.where(lane == e, token, out)
        out = jnp.where(lane == LANES // 2 + e, gate, out)
    pad = jnp.zeros((table.shape[1] - CAP, LANES), F32)
    table[...] = jnp.concatenate([out, pad], axis=0).T


def run_route(ids, logits, cap):
    E, T = logits.shape
    NB = T // LANES
    SP = E + 1 if E % 8 == 0 else E
    wide = -(-cap // LANES) * LANES
    rows = 16 * SP
    return pl.pallas_call(
        functools.partial(route_kernel, (E, T, cap, NB, SP)),
        out_shape=jax.ShapeDtypeStruct((LANES, wide), F32),
        in_specs=[pl.BlockSpec(memory_space=pltpu.VMEM)] * 2,
        out_specs=pl.BlockSpec(memory_space=pltpu.VMEM),
        scratch_shapes=[pltpu.VMEM((rows, LANES), F32)] * 6,
        compiler_params=pltpu.CompilerParams(vmem_limit_bytes=VMEM_ALL),
        cost_estimate=pl.CostEstimate(flops=10_000_000_000, bytes_accessed=2_000_000, transcendentals=0),
        name='route',
    )(ids, logits)


def lists_kernel(cfg, table, lst, gturn, meta, addr):
    S, E, CAP, T, KB, MAXR, WIDE = cfg
    width = table.shape[3]
    lane = lax.broadcasted_iota(jnp.int32, (E, width), 1)
    start = jnp.zeros((E, 1), jnp.int32)
    rows_all = jnp.zeros((E, WIDE), F32)
    gates_all = jnp.zeros((E, WIDE), F32)
    meta_lane = lax.broadcasted_iota(jnp.int32, (E, LANES), 1)
    facts = jnp.zeros((E, LANES), jnp.int32)
    for s in range(S):
        tok = table[0, s]
        gate = table[1, s]
        valid = jnp.logical_and(tok < float(T), lane < CAP)
        cnt = jnp.sum(jnp.where(valid, 1.0, 0.0), axis=1, keepdims=True).astype(jnp.int32)
        addr[s] = jnp.where(valid, tok, float(T)).astype(jnp.int32) * KB
        rows = jnp.where(valid, tok + float(s * T + 1), 0.0)
        gate = jnp.where(valid, gate, 0.0)
        blank = jnp.zeros((E, WIDE - width), F32)
        rows = jnp.concatenate([rows, blank], axis=1)
        gate = jnp.concatenate([gate, blank], axis=1)
        bit = 8
        while bit < MAXR:
            take = (start // bit) % 2 == 1
            rows = jnp.where(take, pltpu.roll(rows, bit, 1), rows)
            gate = jnp.where(take, pltpu.roll(gate, bit, 1), gate)
            bit *= 2
        rows_all = rows_all + rows
        gates_all = gates_all + gate
        facts = jnp.where(meta_lane == s, cnt, facts)
        facts = jnp.where(meta_lane == S + s, start, facts)
        start = start + (cnt + 7) // 8 * 8
    facts = jnp.where(meta_lane == 2 * S, start, facts)
    pad = meta.shape[0] - E
    meta[...] = jnp.concatenate([facts, jnp.zeros((pad, LANES), jnp.int32)], axis=0)
    spread = lax.broadcasted_iota(jnp.int32, (E, WIDE), 1) % (S * T)
    rows_all = jnp.where(rows_all > 0.0, rows_all.astype(jnp.int32) - 1, spread)
    lst[...] = jnp.concatenate([rows_all, jnp.zeros((pad, WIDE), jnp.int32)], axis=0)
    square = jnp.concatenate([gates_all, jnp.zeros((LANES - E, WIDE), F32)], axis=0)
    for c in range(WIDE // LANES):
        cols = slice(c * LANES, (c + 1) * LANES)
        gturn[cols, :] = square[:, cols].T


def run_lists(table, cap, T, KB):
    _, S, E, width = table.shape
    MAXR = S * cap
    WIDE = MAXR + LANES
    rows = E + 8
    vmem = pl.BlockSpec(memory_space=pltpu.VMEM)
    return pl.pallas_call(
        functools.partial(lists_kernel, (S, E, cap, T, KB, MAXR, WIDE)),
        out_shape=(jax.ShapeDtypeStruct((rows, WIDE), jnp.int32), jax.ShapeDtypeStruct((WIDE, LANES), F32), jax.ShapeDtypeStruct((rows, LANES), jnp.int32), jax.ShapeDtypeStruct((S, E, width), jnp.int32)),
        in_specs=[vmem],
        out_specs=(vmem,) * 4,
        compiler_params=pltpu.CompilerParams(vmem_limit_bytes=VMEM_ALL),
        cost_estimate=pl.CostEstimate(flops=10_000_000_000, bytes_accessed=22_000_000, transcendentals=0),
        name='lists',
    )(table)


def attention_kernel(seq, q_ref, k_ref, v_ref, cos_ref, sin_ref, cos_t, sin_t, o_ref):
    step = 128
    half = LANES // 2
    key = lax.broadcasted_iota(jnp.int32, (step, step), 0)
    query = lax.broadcasted_iota(jnp.int32, (step, step), 1)
    keep = query >= key
    factor = LANES ** -0.5 * 1.4426950408889634
    for hh in range(k_ref.shape[1] // LANES):
        at = hh * LANES
        first, second = q_ref[at:at + half, :], q_ref[at + half:at + LANES, :]
        ct, st = cos_t[...], sin_t[...]
        q = jnp.concatenate([first * ct - second * st, second * ct + first * st], axis=0).astype(BF16)
        kf = k_ref[:, at:at + LANES]
        k = (kf * cos_ref[...] + pltpu.roll(kf, half, 1) * sin_ref[...]).astype(BF16)
        v = v_ref[at:at + LANES, :]
        for j in range(seq // step):
            n = (j + 1) * step
            s = jnp.dot(k[:n], q[:, j * step:n], preferred_element_type=F32)
            diag = jnp.where(keep, s[j * step:], NEG)
            s = jnp.concatenate([s[:j * step], diag], axis=0) if j else diag
            p = jnp.exp2((s - jnp.max(s, axis=0, keepdims=True)) * factor)
            p = (p * (1.0 / jnp.sum(p, axis=0, keepdims=True))).astype(BF16)
            o_ref[at:at + LANES, j * step:n] = jnp.dot(v[:, :n], p, preferred_element_type=F32).astype(BF16)


def run_attention(q_t, k, v_t, seq):
    T, D = k.shape
    half = LANES // 2
    freqs = ROPE_BASE ** (-jnp.arange(half, dtype=F32) * 2.0 / LANES)
    angles = jnp.arange(seq, dtype=F32)[:, None] * freqs[None, :]
    cos_half, sin_half = jnp.cos(angles), jnp.sin(angles)
    cosine = jnp.concatenate([cos_half, cos_half], axis=1)
    sine = jnp.concatenate([-sin_half, sin_half], axis=1)
    wide = min(D, 512)
    block = pl.BlockSpec((seq, wide), lambda i, j: (i, j))
    block_t = pl.BlockSpec((wide, seq), lambda i, j: (j, i))
    table = pl.BlockSpec((seq, LANES), lambda i, j: (0, 0))
    table_t = pl.BlockSpec((half, seq), lambda i, j: (0, 0))
    return pl.pallas_call(
        functools.partial(attention_kernel, seq),
        grid=(T // seq, D // wide),
        out_shape=jax.ShapeDtypeStruct((D, T), BF16),
        in_specs=[block_t, block, block_t, table, table, table_t, table_t],
        out_specs=block_t,
        compiler_params=pltpu.CompilerParams(vmem_limit_bytes=VMEM_ALL),
        cost_estimate=pl.CostEstimate(flops=50_000_000_000, bytes_accessed=76_000_000, transcendentals=0),
        name='attention',
    )(q_t, k, v_t, cosine, sine, cos_half.T, sin_half.T)


def final_kernel(KB, b, m, *rest):
    o = rest[-1]
    rows = b.shape[0]
    for k in range(KB):
        cols = slice(k * LANES, (k + 1) * LANES)
        o[:, cols] = (b[:, cols] + m[pl.ds(k, rows, stride=KB), :]).astype(BF16)


def run_final(low, high, rows, b, m, earlier):
    total, D = b.shape
    KB = D // LANES
    first = low // rows
    args = [b, m]
    specs = [pl.BlockSpec((rows, D), lambda i: (first + i, 0)), pl.BlockSpec((rows * KB, LANES), lambda i: (i, 0))]
    aliases = {}
    if earlier is not None:
        args.append(earlier)
        specs.append(pl.BlockSpec(memory_space=pl.ANY))
        aliases = {2: 0}
    return pl.pallas_call(
        functools.partial(final_kernel, KB),
        grid=((high - low) // rows,),
        out_shape=jax.ShapeDtypeStruct((total, D), BF16),
        in_specs=specs,
        out_specs=pl.BlockSpec((rows, D), lambda i: (first + i, 0)),
        input_output_aliases=aliases,
        compiler_params=pltpu.CompilerParams(vmem_limit_bytes=VMEM_ALL),
        cost_estimate=pl.CostEstimate(flops=1_000_000_000, bytes_accessed=32_000_000, transcendentals=0),
        name='final',
    )(*args)


def run_experts(meta, lst, gates, u, own, other):
    E, MAXR = 2 * own[0].shape[0], gates.shape[0] - LANES
    D, FE = own[0].shape[1], own[0].shape[2]
    KB = D // LANES
    sizes = (256, 320, 384)
    limit = min(MAXR, 1152)
    cfg = (E, KB, FE, MAXR, lst.shape[1], limit, sizes)
    entries = E * -(-MAXR // limit) + 2
    any_spec = pl.BlockSpec(memory_space=pl.ANY)
    smem = pl.BlockSpec(memory_space=pltpu.SMEM)
    return pl.pallas_call(
        functools.partial(expert_kernel, cfg),
        out_shape=jax.ShapeDtypeStruct(((E * MAXR + 32) // 8 * KB * PITCH, LANES), F32),
        in_specs=[smem, smem, pl.BlockSpec(memory_space=pltpu.VMEM)] + [any_spec] * 7,
        out_specs=any_spec,
        scratch_shapes=[
            pltpu.VMEM((2, D, FE), BF16), pltpu.VMEM((2, D, FE), BF16), pltpu.VMEM((2, FE, D), BF16),
            pltpu.VMEM((SLOTS * limit, KB, LANES), BF16), pltpu.VMEM((32 * (KB + 1), LANES), F32), pltpu.VMEM((max(sizes) // 16, KB, 16, LANES), BF16),
            pltpu.VMEM((max(sizes), FE), BF16), pltpu.VMEM((2 * max(sizes) // 8 * KB * PITCH, LANES), F32), pltpu.SMEM((4,), jnp.int32), pltpu.SMEM((SLOTS,), jnp.int32), pltpu.SMEM((3 * entries,), jnp.int32),
            pltpu.SemaphoreType.DMA((2,)), pltpu.SemaphoreType.DMA((SLOTS,)), pltpu.SemaphoreType.DMA((2,)),
        ],
        compiler_params=pltpu.CompilerParams(vmem_limit_bytes=VMEM_ALL),
        cost_estimate=pl.CostEstimate(flops=E * MAXR * D * FE * 3, bytes_accessed=400_000_000, transcendentals=0),
        name='experts',
    )(meta.reshape(-1), lst.reshape(-1), gates, u, *own, *other)


def run_combine(meta, addr, y, T, KB, cap):
    chips, E, width = addr.shape
    MAXR = chips * cap
    DEPTH = 4
    cfg = (E, chips, cap, KB, MAXR, T, DEPTH, width)
    smem = pl.BlockSpec(memory_space=pltpu.SMEM)
    any_spec = pl.BlockSpec(memory_space=pl.ANY)
    return pl.pallas_call(
        functools.partial(combine_kernel, cfg),
        out_shape=jax.ShapeDtypeStruct((chips, T * KB, LANES), F32),
        in_specs=[smem, smem, any_spec],
        out_specs=any_spec,
        scratch_shapes=[
            pltpu.VMEM((2, (T + 8) * KB, LANES), F32), pltpu.VMEM((DEPTH * (cap // 8) * KB * PITCH, LANES), F32),
            pltpu.SemaphoreType.DMA((DEPTH,)), pltpu.SemaphoreType.DMA((2,)),
        ],
        compiler_params=pltpu.CompilerParams(vmem_limit_bytes=VMEM_ALL),
        cost_estimate=pl.CostEstimate(flops=40_000_000_000, bytes_accessed=150_000_000, transcendentals=0),
        name='combine',
    )(meta.reshape(-1), addr.reshape(-1), y)


def solution(mesh):
    group_size = mesh.shape['ep']
    tok_spec = P(None, ('dp', 'ep'), None, None)
    rep_one = P(None)
    rep_two = P(None, None)
    rep_three = P(None, None, None)
    expert_spec = P('ep', None, None)
    chips = group_size // 2
    same_core = [[2 * c for c in range(chips)], [2 * c + 1 for c in range(chips)]]
    partner = [(i, i ^ 1) for i in range(group_size)]

    def local_program(resid_in, expert_idx, expert_slot, w_query, w_key, w_value, w_out, w_gate, w_up, w_down, w_router, norm_attn, norm_ffn, norm_moe, expert_gate, expert_up, expert_down):
        micros, seqs, seq_len, width = resid_in.shape
        T = seqs * seq_len
        KB = width // LANES
        choices = expert_idx.shape[-1]
        local_experts = expert_gate.shape[0]
        experts = local_experts * group_size
        E = 2 * local_experts
        cap = CAP_FACTOR * T * choices // experts
        me = lax.axis_index('ep')
        own = (expert_gate, expert_up, expert_down)
        other = tuple(lax.ppermute(w, 'ep', partner) for w in own)

        total = micros * T
        resid = resid_in.reshape(total, width)
        rows = min(256, T // 2)
        split = int(total * FIRST_SHARE) // rows * rows
        chunks = []
        for low, high in ((0, split), (split, total)):
            held = sum(min(cap, max(0, min(high, (m + 1) * T) - max(low, m * T))) for m in range(micros))
            chunks.append((low, high, held))
        router_t = w_router.T
        tokens_all, nattn, logits = [], None, None
        for low, high, _ in chunks:
            u3, nattn, logits = run_prep(low, high, rows, resid, norm_moe, norm_attn, router_t, (nattn, logits) if low else None)
            tokens_all.append(lax.all_gather(u3, 'ep', axis_index_groups=same_core))
        ids = expert_idx.reshape(total, choices).T
        tables = [run_route(ids[:, low:high], logits[:, low:high], held) for low, high, held in chunks]
        widths = [t.shape[1] for t in tables]
        table = jnp.concatenate(tables, axis=1).reshape(2, LANES // 2, -1)[:, :experts].reshape(2, chips, E, -1)
        table = lax.all_to_all(table, 'ep', 1, 1, tiled=True, axis_index_groups=same_core)
        core = lax.rem(me, 2)
        table = jnp.concatenate([lax.dynamic_slice_in_dim(table, core * local_experts, local_experts, 2), lax.dynamic_slice_in_dim(table, (1 - core) * local_experts, local_experts, 2)], 2)
        plans, at = [], 0
        for (low, high, held), wide in zip(chunks, widths):
            plans.append(run_lists(table[:, :, :, at:at + wide], held, high - low, KB))
            at += wide

        across = (((0,), (1,)), ((), ()))
        q_t = lax.dot_general(w_query.reshape(width, -1), nattn, across, preferred_element_type=F32)
        k = jnp.dot(nattn, w_key.reshape(width, -1), preferred_element_type=F32)
        v_t = lax.dot_general(w_value.reshape(width, -1), nattn, across, preferred_element_type=F32).astype(BF16)

        o_t = run_attention(q_t, k, v_t, seq_len)

        summed = []
        for (low, high, held), tokens, (lst, gates, meta, addr) in zip(chunks, tokens_all, plans):
            count = high - low
            if low == 0:
                meta, o_t = lax.optimization_barrier((meta, o_t))
            y = run_experts(meta, lst, gates, tokens.reshape(chips * count, KB, LANES), own, other)
            part = run_combine(meta, addr, y, count, KB, held)
            if high == total:
                part, o_t = lax.optimization_barrier((part, o_t))
            summed.append(lax.psum_scatter(part, 'ep', scatter_dimension=0, axis_index_groups=same_core))
        attn_out = lax.dot_general(o_t, w_out.reshape(-1, width), (((0,), (0,)), ((), ())), preferred_element_type=F32)
        after = (resid.astype(F32) + attn_out).astype(BF16)
        dense = ffn_branch(after, norm_ffn, w_gate, w_up, w_down)
        out = None
        for (low, high, _), moe in zip(chunks, summed):
            out = run_final(low, high, rows, dense, moe.reshape((high - low) * KB, LANES), out)
        return out.reshape(micros, seqs, seq_len, width)

    return jax.shard_map(local_program, mesh=mesh, in_specs=(tok_spec, tok_spec, tok_spec, rep_three, rep_three, rep_three, rep_three, rep_two, rep_two, rep_two, rep_two, rep_one, rep_one, rep_one, expert_spec, expert_spec, expert_spec), out_specs=tok_spec, check_vma=False)
```
